128 devices in a mesh: data: 1, model: 2 (over core), seq: 64 (over z, y, x).
Axes of the slice: x: 4, y: 4, z: 4, core: 2. Of those that a mesh axis runs over, the one named last changes fastest.
Arguments:
- tokens: bfloat16 [8, 98304, 384], P('data', 'seq')
- lengths: int32 [8], P('data')
- slot_params: bfloat16 [384, 128], replicated
- logit_scale: float32 [], replicated
- w_in: bfloat16 [128, 384, 1536], P('seq', None, 'model')
- w_out: bfloat16 [128, 1536, 384], P('seq', 'model')
Outputs:
- output: bfloat16 [8, 98304, 384], P('data', 'seq')
All inputs are finite; a program needn't handle non-finite values.
Results may differ from the reference program's by a relative error of at most 0.0163054.
Values are sent between devices in bfloat16 or wider.
A program may use at most 1 GiB of HBM per device.

```python
import math
import jax
import jax.numpy as jnp
from jax import lax

BATCH_SIZE = 8
SEQ_LEN = 98304
MODEL_DIM = 384
HIDDEN_DIM = 1536
NUM_EXPERTS = 128
EXPERT_SLOTS = 1
NUM_SLOTS_TOTAL = NUM_EXPERTS * EXPERT_SLOTS
NORM_EPS = 1e-6


def setup_inputs(seed: int = 0, part: int = 0) -> dict:
    root_key = jax.random.key(seed)
    key_phi, key_gain, key_win, key_wout, key_part = jax.random.split(root_key, 5)
    part_key = jax.random.fold_in(key_part, part)
    key_tok, key_len = jax.random.split(part_key, 2)
    tokens = jax.random.normal(key_tok, (BATCH_SIZE, SEQ_LEN, MODEL_DIM), jnp.float32).astype(jnp.bfloat16)
    drawn = jax.random.randint(key_len, (BATCH_SIZE,), SEQ_LEN // 4, SEQ_LEN + 1, jnp.int32)
    lengths = jnp.where(jnp.arange(BATCH_SIZE) == 0, SEQ_LEN, drawn).astype(jnp.int32)
    slot_params = jax.random.normal(key_phi, (MODEL_DIM, NUM_SLOTS_TOTAL), jnp.float32).astype(jnp.bfloat16)
    logit_scale = math.sqrt(MODEL_DIM) * jax.random.uniform(key_gain, (), jnp.float32, 1.0, 2.0)
    in_scale = math.sqrt(SEQ_LEN) / (4.0 * math.sqrt(MODEL_DIM))
    w_in = (jax.random.normal(key_win, (NUM_EXPERTS, MODEL_DIM, HIDDEN_DIM), jnp.float32) * in_scale).astype(jnp.bfloat16)
    w_out = (jax.random.normal(key_wout, (NUM_EXPERTS, HIDDEN_DIM, MODEL_DIM), jnp.float32) / math.sqrt(HIDDEN_DIM)).astype(jnp.bfloat16)
    return {"tokens": tokens, "lengths": lengths, "slot_params": slot_params, "logit_scale": logit_scale, "w_in": w_in, "w_out": w_out}


def unit_vectors(values, axis):
    v32 = values.astype(jnp.float32)
    return (v32 * lax.rsqrt(jnp.sum(v32 * v32, axis=axis, keepdims=True) + NORM_EPS)).astype(jnp.bfloat16)


def reference(tokens, lengths, slot_params, logit_scale, w_in, w_out):
    slot_unit = unit_vectors(slot_params, 0)
    positions = jnp.arange(SEQ_LEN)

    def seq_logits(seq_tokens):
        return logit_scale * jnp.dot(unit_vectors(seq_tokens, 1), slot_unit, preferred_element_type=jnp.float32)

    def dispatch(args):
        seq_tokens, seq_length = args
        logits = seq_logits(seq_tokens)
        masked = jnp.where((positions < seq_length)[:, None], logits, -1e30)
        weights = jnp.exp(masked - jnp.max(masked, axis=0, keepdims=True))
        col_sum = jnp.sum(weights, axis=0)
        slot_sum = jnp.dot(weights.astype(jnp.bfloat16).T, seq_tokens, preferred_element_type=jnp.float32)
        return (slot_sum / col_sum[:, None]).astype(jnp.bfloat16)

    slot_in = lax.map(dispatch, (tokens, lengths))
    per_expert = slot_in.reshape(BATCH_SIZE, NUM_EXPERTS, EXPERT_SLOTS, MODEL_DIM).transpose(1, 0, 2, 3).reshape(NUM_EXPERTS, BATCH_SIZE * EXPERT_SLOTS, MODEL_DIM)

    def expert_ffn(args):
        rows, first, second = args
        hidden = jax.nn.gelu(jnp.dot(rows, first, preferred_element_type=jnp.float32), approximate=False).astype(jnp.bfloat16)
        return jnp.dot(hidden, second, preferred_element_type=jnp.float32).astype(jnp.bfloat16)

    expert_out = lax.map(expert_ffn, (per_expert, w_in, w_out))
    slot_out = expert_out.reshape(NUM_EXPERTS, BATCH_SIZE, EXPERT_SLOTS, MODEL_DIM).transpose(1, 0, 2, 3).reshape(BATCH_SIZE, NUM_SLOTS_TOTAL, MODEL_DIM)

    def combine(args):
        seq_tokens, seq_length, seq_slots = args
        mix_weights = jax.nn.softmax(seq_logits(seq_tokens), axis=1).astype(jnp.bfloat16)
        mixed = jnp.dot(mix_weights, seq_slots, preferred_element_type=jnp.float32)
        return jnp.where((positions < seq_length)[:, None], mixed, 0.0).astype(jnp.bfloat16)

    return lax.map(combine, (tokens, lengths, slot_out))
```

```python
import functools

import jax
import jax.numpy as jnp
from jax import lax
from jax.experimental import pallas as pl
from jax.experimental.pallas import tpu as pltpu
from jax.sharding import PartitionSpec as P

NORM_EPS = 1e-6
MESH = pl.DeviceIdType.MESH
SIDE = 4
F32, BF16 = jnp.float32, jnp.bfloat16
NEG = -1e30


def dot(a, b, ca, cb):
    return lax.dot_general(a, b, (((ca,), (cb,)), ((), ())), preferred_element_type=F32)


def moe_kernel(lens, scale, phi, x_hbm, win_hbm, wout_hbm, c_hbm, slots_hbm,
               x_v, win_v, wout_v, c_v, u_v, v_v, vt_v, tmp_v, lt_v, w_v, pack_v, send_v, recv_v,
               xs_v, part_v, peer_v, ys_v, ag_v, unpack_v, slots_v,
               x_sem, w_sem, c_sem, s_sem, sems):
    n_batch, toks, dim = x_hbm.shape
    half = n_batch // 2
    slots = phi.shape[1]
    chips = slots // 2
    core = lax.axis_index("model")
    chip = lax.axis_index("seq")
    cz, cy, cx = chip // (SIDE * SIDE), (chip // SIDE) % SIDE, chip % SIDE
    first = core * half
    other = 1 - core

    def batch_of(q):
        return lax.rem(first + q, n_batch)

    def x_copy(q):
        return pltpu.make_async_copy(x_hbm.at[batch_of(q)], x_v.at[q], x_sem.at[q])

    for q in range(n_batch):
        x_copy(q).start()
    win_copy = pltpu.make_async_copy(win_hbm, win_v, w_sem.at[0])
    wout_copy = pltpu.make_async_copy(wout_hbm, wout_v, w_sem.at[1])
    win_copy.start()
    wout_copy.start()

    def peer(r):
        dz, dy, dx = r // (SIDE * SIDE), (r // SIDE) % SIDE, r % SIDE
        return ((cz + dz) % SIDE) * (SIDE * SIDE) + ((cy + dy) % SIDE) * SIDE + (cx + dx) % SIDE

    barrier = pltpu.get_barrier_semaphore()
    pl.semaphore_signal(barrier, inc=1, device_id={"model": other}, device_id_type=MESH)

    @pl.loop(1, chips)
    def _(r):
        pl.semaphore_signal(barrier, inc=1, device_id={"seq": peer(r)}, device_id_type=MESH)

    g = scale[0]

    p32 = phi[...].astype(F32)
    unit = (p32 * lax.rsqrt(jnp.sum(p32 * p32, axis=0, keepdims=True) + NORM_EPS))
    for d in range(dim // 128):
        cols = slice(d * 128, (d + 1) * 128)
        tmp_v[d] = unit[cols, :].T
        for k in range(2):
            vt_v[k * chips:(k + 1) * chips, cols] = tmp_v[d, pl.ds(k, chips, stride=2), :].astype(BF16)
    v_v[...] = vt_v[...].astype(F32).T.astype(BF16)

    rows = 256

    def unit_rows(q):
        for t in range(toks // rows):
            part = x_v[q, t * rows:(t + 1) * rows, :].astype(F32)
            norm = lax.rsqrt(jnp.sum(part * part, axis=1, keepdims=True) + NORM_EPS)
            u_v[t * rows:(t + 1) * rows, :] = (part * norm).astype(BF16)

    lane = lax.broadcasted_iota(jnp.int32, (slots, 128), 1)

    @pl.loop(0, half)
    def _(q):
        x_copy(q).wait()
        unit_rows(q)
        left = lens[batch_of(q)] - chip * toks
        top = jnp.full((slots, rows), NEG, F32)
        for t in range(toks // rows):
            span = slice(t * rows, (t + 1) * rows)
            lg = g * dot(vt_v[...], u_v[span, :], 1, 1)
            pos = lax.broadcasted_iota(jnp.int32, lg.shape, 1) + t * rows
            lg = jnp.where(pos < left, lg, NEG)
            lt_v[:, span] = lg
            top = jnp.maximum(top, lg)
        top = jnp.max(top, axis=1, keepdims=True)
        total = jnp.zeros((slots, rows), F32)
        for t in range(toks // rows):
            span = slice(t * rows, (t + 1) * rows)
            w = jnp.exp(lt_v[:, span] - top)
            total = total + w
            w_v[:, span] = w.astype(BF16)
        total = jnp.sum(total, axis=1, keepdims=True)
        sums = dot(w_v[...], x_v[q], 1, 0)
        stat = jnp.zeros((slots, 128), F32)
        for pos, val in ((0, top), (3, total)):
            rest = val
            for i in range(3):
                piece = rest.astype(BF16).astype(F32)
                rest = rest - piece
                stat = jnp.where(lane == pos + i, piece, stat)
        for k in range(2):
            dst = pl.ds(2 * q + k, chips, stride=2 * half)
            for d in range(dim // 128):
                pack_v[d, dst, :] = sums[k * chips:(k + 1) * chips, d * 128:(d + 1) * 128]
            pack_v[dim // 128, dst, :] = stat[k * chips:(k + 1) * chips, :]

    for d in range(dim // 128 + 1):
        send_v[:, :, d * 128:(d + 1) * 128] = pack_v[d].astype(BF16).reshape(chips, 2 * half, 128)
    recv_v[0] = send_v[chip]

    pl.semaphore_wait(barrier, chips)

    @pl.loop(1, chips)
    def _(r):
        to = peer(r)
        pltpu.make_async_remote_copy(send_v.at[to], recv_v.at[r], sems.at[0], sems.at[1], device_id={"seq": to}, device_id_type=MESH).start()

    def mix_weights(q):
        unit_rows(q)
        for t in range(toks // rows):
            span = slice(t * rows, (t + 1) * rows)
            lg = g * dot(u_v[span, :], v_v[...], 1, 0)
            e = jnp.exp(lg - jnp.max(lg, axis=1, keepdims=True))
            c_v[q, span, :] = (e / jnp.sum(e, axis=1, keepdims=True)).astype(BF16)
        pltpu.make_async_copy(c_v.at[q], c_hbm.at[batch_of(q)], c_sem).start()

    @pl.loop(0, half)
    def _(q):
        mix_weights(q)

    arrived = recv_v.at[pl.ds(1, chips - 1)]
    pltpu.make_async_copy(arrived, arrived, sems.at[1]).wait()
    n_rows = 2 * half
    got = recv_v[:, :, dim:].reshape(chips * n_rows, 128)
    sel_row = lax.broadcasted_iota(jnp.int32, (128, 128), 0)
    tops = dot(got, (sel_row < 3).astype(F32).astype(BF16), 1, 0).reshape(chips, n_rows, 128)
    totals = dot(got, ((sel_row >= 3) & (sel_row < 6)).astype(F32).astype(BF16), 1, 0).reshape(chips, n_rows, 128)
    factor = jnp.exp(tops - jnp.max(tops, axis=0, keepdims=True))
    z = jnp.sum(factor * totals, axis=0)
    for d in range(dim // 128):
        cols = slice(d * 128, (d + 1) * 128)
        acc = jnp.sum(factor * recv_v[:, :, cols].astype(F32), axis=0)
        xs_v[core, :, cols] = (acc / z).astype(BF16)

    def to_partner(src, dst, i):
        return pltpu.make_async_remote_copy(src, dst, sems.at[i], sems.at[i + 1], device_id={"model": other}, device_id_type=MESH)

    xs_copy = to_partner(xs_v.at[core], xs_v.at[core], 2)
    xs_copy.start()
    win_copy.wait()
    wout_copy.wait()
    xs_copy.wait()

    ins = xs_v[...].reshape(2 * n_rows, dim)
    parity = lax.broadcasted_iota(jnp.int32, (2 * n_rows, dim), 0) % 2
    out = None
    for k in range(2):
        hid = dot(ins, win_v[k], 1, 0)
        hid = (0.5 * hid * (1.0 + lax.erf(hid * 0.7071067811865476))).astype(BF16)
        res = dot(hid, wout_v[k], 1, 0)
        out = res if out is None else jnp.where(parity == k, res, out)
    part_v[...] = out.reshape(2, n_rows, dim)
    part_copy = to_partner(part_v.at[other], peer_v, 4)
    part_copy.start()
    part_copy.wait()
    ys_v[...] = (part_v[core] + peer_v[...]).astype(BF16)
    ag_v[0] = ys_v[...]

    @pl.loop(1, chips)
    def _(r):
        pltpu.make_async_remote_copy(ys_v, ag_v.at[r], sems.at[6], sems.at[7], device_id={"seq": peer(r)}, device_id_type=MESH).start()

    @pl.loop(half, n_batch)
    def _(q):
        x_copy(q).wait()
        mix_weights(q)

    arrived = ag_v.at[pl.ds(1, chips - 1)]
    pltpu.make_async_copy(arrived, arrived, sems.at[7]).wait()

    @pl.loop(0, chips)
    def _(s):
        sz, sy, sx = s // (SIDE * SIDE), (s // SIDE) % SIDE, s % SIDE
        r = ((cz - sz + SIDE) % SIDE) * (SIDE * SIDE) + ((cy - sy + SIDE) % SIDE) * SIDE + (cx - sx + SIDE) % SIDE
        for d in range(dim // 128):
            unpack_v[d, pl.ds(pl.multiple_of(s * n_rows, n_rows), n_rows), :] = ag_v[r, :, d * 128:(d + 1) * 128].astype(F32)

    for i in range(half):
        for k in range(2):
            for d in range(dim // 128):
                slots_v[i, k * chips:(k + 1) * chips, d * 128:(d + 1) * 128] = unpack_v[d, pl.ds(2 * i + k, chips, stride=n_rows), :].astype(BF16)

    mine = slots_hbm.at[pl.ds(first, half)]
    keep = pltpu.make_async_copy(slots_v, mine, s_sem)
    give = to_partner(slots_v, mine, 8)
    keep.start()
    give.start()
    sent = send_v.at[pl.ds(1, chips - 1)]
    pltpu.make_async_copy(sent, sent, sems.at[0]).wait()
    sent = ag_v.at[pl.ds(1, chips - 1)]
    pltpu.make_async_copy(sent, sent, sems.at[6]).wait()
    pltpu.make_async_copy(c_v, c_hbm, c_sem).wait()
    keep.wait()
    give.wait()


def mix_kernel(lens, c, slots, y):
    left = lens[pl.program_id(0)] - lax.axis_index("seq") * c.shape[1]
    rows = 256
    for t in range(c.shape[1] // rows):
        span = slice(t * rows, (t + 1) * rows)
        out = dot(c[0, span, :], slots[0], 1, 0)
        pos = lax.broadcasted_iota(jnp.int32, out.shape, 0) + t * rows
        y[0, span, :] = jnp.where(pos < left, out, 0.0).astype(BF16)


def solution(mesh):
    def local_layer(tokens, lengths, slot_params, logit_scale, w_in, w_out):
        n_batch, toks, dim = tokens.shape
        slots = slot_params.shape[1]
        chips, half = slots // 2, n_batch // 2
        n_rows = 2 * half
        smem = pl.BlockSpec(memory_space=pltpu.SMEM)
        vmem = pl.BlockSpec(memory_space=pltpu.VMEM)
        hbm = pl.BlockSpec(memory_space=pl.ANY)
        dma = pltpu.SemaphoreType.DMA
        weights, slot_out = pl.pallas_call(
            moe_kernel,
            name="moe",
            out_shape=(jax.ShapeDtypeStruct((n_batch, toks, slots), BF16), jax.ShapeDtypeStruct((n_batch, slots, dim), BF16)),
            in_specs=[smem, smem, vmem, hbm, hbm, hbm],
            out_specs=(hbm, hbm),
            scratch_shapes=[
                pltpu.VMEM((n_batch, toks, dim), BF16),
                pltpu.VMEM(w_in.shape, BF16),
                pltpu.VMEM(w_out.shape, BF16),
                pltpu.VMEM((n_batch, toks, slots), BF16),
                pltpu.VMEM((toks, dim), BF16),
                pltpu.VMEM((dim, slots), BF16),
                pltpu.VMEM((slots, dim), BF16),
                pltpu.VMEM((dim // 128, slots, 128), F32),
                pltpu.VMEM((slots, toks), F32),
                pltpu.VMEM((slots, toks), BF16),
                pltpu.VMEM((dim // 128 + 1, chips * n_rows, 128), F32),
                pltpu.VMEM((chips, n_rows, dim + 128), BF16),
                pltpu.VMEM((chips, n_rows, dim + 128), BF16),
                pltpu.VMEM((2, n_rows, dim), BF16),
                pltpu.VMEM((2, n_rows, dim), F32),
                pltpu.VMEM((n_rows, dim), F32),
                pltpu.VMEM((n_rows, dim), BF16),
                pltpu.VMEM((chips, n_rows, dim), BF16),
                pltpu.VMEM((dim // 128, chips * n_rows, 128), F32),
                pltpu.VMEM((half, slots, dim), BF16),
                dma((n_batch,)), dma((2,)), dma, dma, dma((10,)),
            ],
            compiler_params=pltpu.CompilerParams(collective_id=0, has_side_effects=True, vmem_limit_bytes=58 * 2**20),
        )(lengths, logit_scale.reshape(1), slot_params, tokens, w_in, w_out)
        return pl.pallas_call(
            mix_kernel,
            name="mix",
            out_shape=jax.ShapeDtypeStruct(tokens.shape, BF16),
            grid=(n_batch,),
            in_specs=[smem, pl.BlockSpec((1, toks, slots), lambda b: (b, 0, 0)), pl.BlockSpec((1, slots, dim), lambda b: (b, 0, 0))],
            out_specs=pl.BlockSpec((1, toks, dim), lambda b: (b, 0, 0)),
            compiler_params=pltpu.CompilerParams(dimension_semantics=("arbitrary",)),
        )(lengths, weights, slot_out)

    return jax.shard_map(local_layer, mesh=mesh, in_specs=(P("data", "seq", None), P("data"), P(), P(), P("seq", None, "model"), P("seq", "model", None)), out_specs=P("data", "seq", None), check_vma=False)
```

```python
import jax
import jax.numpy as jnp
from jax import lax
from jax.experimental import pallas as pl
from jax.experimental.pallas import tpu as pltpu
from jax.sharding import PartitionSpec as P

NORM_EPS = 1e-6
MESH = pl.DeviceIdType.MESH
SIDE = 4
F32, BF16 = jnp.float32, jnp.bfloat16
NEG = -1e30
scope = jax.named_scope


def dot(a, b, ca, cb):
    return lax.dot_general(a, b, (((ca,), (cb,)), ((), ())), preferred_element_type=F32)


def far_first():
    near = (0, 1, 2, 1)
    every = [(z, y, x) for z in range(SIDE) for y in range(SIDE) for x in range(SIDE)]
    return sorted(every[1:], key=lambda o: (-sum(near[i] for i in o), o))


def moe_kernel(lens_hbm, scale, phi_hbm, x_hbm, win_hbm, wout_hbm, c_v, slots_v, left_v,
               lens, phi, x_v, win_v, wout_v, u_v, v_v, vt_v, tmp_v, lt_v, w_v, pack_v, send_v, recv_v,
               xs_v, part_v, peer_v, ys_v, ag_v, unpack_v,
               x_sem, l_sem, sems):
    n_batch, toks, dim = x_hbm.shape
    half = n_batch // 2
    slots = phi.shape[1]
    chips = slots // 2
    core = lax.axis_index("model")
    chip = lax.axis_index("seq")
    cz, cy, cx = chip // (SIDE * SIDE), (chip // SIDE) % SIDE, chip % SIDE
    first = core * half
    other = 1 - core

    def batch_of(q):
        return lax.rem(first + q, n_batch)

    def x_copy(q):
        return pltpu.make_async_copy(x_hbm.at[batch_of(q)], x_v.at[q], x_sem.at[q])

    loads = [pltpu.make_async_copy(a, b, l_sem.at[i]) for i, (a, b) in enumerate(
        ((phi_hbm, phi), (lens_hbm, lens), (win_hbm, win_v), (wout_hbm, wout_v)))]
    for load in loads[:2]:
        load.start()
    for q in range(n_batch):
        x_copy(q).start()
    for load in loads[2:]:
        load.start()

    at_z = [(cz + d) % SIDE * (SIDE * SIDE) for d in range(SIDE)]
    at_y = [(cy + d) % SIDE * SIDE for d in range(SIDE)]
    at_x = [(cx + d) % SIDE for d in range(SIDE)]
    peers = [at_z[z] + at_y[y] + at_x[x] for z, y, x in far_first()]

    with scope("signal"):
        barrier = pltpu.get_barrier_semaphore()
        for to in peers:
            pl.semaphore_signal(barrier, inc=1, device_id={"seq": to}, device_id_type=MESH)
        pl.semaphore_signal(barrier, inc=1, device_id={"model": other}, device_id_type=MESH)

    with scope("phi"):
        for load in loads[:2]:
            load.wait()
        g = scale[...]
        p32 = phi[...].astype(F32)
        unit = (p32 * lax.rsqrt(jnp.sum(p32 * p32, axis=0, keepdims=True) + NORM_EPS))
        for d in range(dim // 128):
            cols = slice(d * 128, (d + 1) * 128)
            tmp_v[d] = unit[cols, :].T
            for k in range(2):
                vt_v[k * chips:(k + 1) * chips, cols] = tmp_v[d, pl.ds(k, chips, stride=2), :].astype(BF16)
        v_v[...] = vt_v[...].astype(F32).T.astype(BF16)
        for b in range(n_batch):
            left_v[b:b + 1, :] = jnp.full((1, 128), lens[b] - chip * toks, jnp.int32)

    rows = 256

    def unit_rows(q):
        for t in range(toks // rows):
            part = x_v[q, t * rows:(t + 1) * rows, :].astype(F32)
            norm = lax.rsqrt(jnp.sum(part * part, axis=1, keepdims=True) + NORM_EPS)
            u_v[t * rows:(t + 1) * rows, :] = (part * norm).astype(BF16)

    lane = lax.broadcasted_iota(jnp.int32, (slots, 128), 1)

    def dispatch(q):
        x_copy(q).wait()
        unit_rows(q)
        left = lens[batch_of(q)] - chip * toks
        top = jnp.full((slots, rows), NEG, F32)
        for t in range(toks // rows):
            span = slice(t * rows, (t + 1) * rows)
            lg = g * dot(vt_v[...], u_v[span, :], 1, 1)
            pos = lax.broadcasted_iota(jnp.int32, lg.shape, 1) + t * rows
            lg = jnp.where(pos < left, lg, NEG)
            lt_v[:, span] = lg
            top = jnp.maximum(top, lg)
        top = jnp.max(top, axis=1, keepdims=True)
        total = jnp.zeros((slots, rows), F32)
        for t in range(toks // rows):
            span = slice(t * rows, (t + 1) * rows)
            w = jnp.exp(lt_v[:, span] - top)
            total = total + w
            w_v[:, span] = w.astype(BF16)
        total = jnp.sum(total, axis=1, keepdims=True)
        sums = dot(w_v[...], x_v[q], 1, 0)
        stat = jnp.zeros((slots, 128), F32)
        for pos, val in ((0, top), (3, total)):
            rest = val
            for i in range(3):
                piece = rest.astype(BF16).astype(F32)
                rest = rest - piece
                stat = jnp.where(lane == pos + i, piece, stat)
        for k in range(2):
            dst = pl.ds(2 * q + k, chips, stride=2 * half)
            for d in range(dim // 128):
                pack_v[d, dst, :] = sums[k * chips:(k + 1) * chips, d * 128:(d + 1) * 128]
            pack_v[dim // 128, dst, :] = stat[k * chips:(k + 1) * chips, :]

    with scope("dispatch"):
        @pl.loop(0, half)
        def _(q):
            dispatch(q)

    with scope("pack"):
        for d in range(dim // 128 + 1):
            send_v[:, :, d * 128:(d + 1) * 128] = pack_v[d].astype(BF16).reshape(chips, 2 * half, 128)
        recv_v[chip] = send_v[chip]

    with scope("barrier"):
        pl.semaphore_wait(barrier, chips)

    with scope("send"):
        for to in peers:
            pltpu.make_async_remote_copy(send_v.at[to], recv_v.at[chip], sems.at[0], sems.at[1], device_id={"seq": to}, device_id_type=MESH).start()

    def mix_weights(q):
        unit_rows(q)
        b = batch_of(q)
        for t in range(toks // rows):
            span = slice(t * rows, (t + 1) * rows)
            lg = g * dot(u_v[span, :], v_v[...], 1, 0)
            e = jnp.exp(lg - jnp.max(lg, axis=1, keepdims=True))
            c_v[b, span, :] = (e / jnp.sum(e, axis=1, keepdims=True)).astype(BF16)

    with scope("mix1"):
        @pl.loop(0, half)
        def _(q):
            mix_weights(q)

    with scope("wait_a2a"):
        arrived = recv_v.at[pl.ds(1, chips - 1)]
        pltpu.make_async_copy(arrived, arrived, sems.at[1]).wait()

    n_rows = 2 * half
    with scope("meet"):
        got = recv_v[:, :, dim:].reshape(chips * n_rows, 128)
        sel_row = lax.broadcasted_iota(jnp.int32, (128, 128), 0)
        tops = dot(got, (sel_row < 3).astype(F32).astype(BF16), 1, 0).reshape(chips, n_rows, 128)
        totals = dot(got, ((sel_row >= 3) & (sel_row < 6)).astype(F32).astype(BF16), 1, 0).reshape(chips, n_rows, 128)
        factor = jnp.exp(tops - jnp.max(tops, axis=0, keepdims=True))
        z = jnp.sum(factor * totals, axis=0)
        for d in range(dim // 128):
            cols = slice(d * 128, (d + 1) * 128)
            acc = jnp.sum(factor * recv_v[:, :, cols].astype(F32), axis=0)
            xs_v[core, :, cols] = (acc / z).astype(BF16)

    def to_partner(src, dst, i):
        return pltpu.make_async_remote_copy(src, dst, sems.at[i], sems.at[i + 1], device_id={"model": other}, device_id_type=MESH)

    with scope("xs_exchange"):
        xs_copy = to_partner(xs_v.at[core], xs_v.at[core], 2)
        xs_copy.start()
        for load in loads[2:]:
            load.wait()
        xs_copy.wait()

    with scope("ffn"):
        ins = xs_v[...].reshape(2 * n_rows, dim)
        parity = lax.broadcasted_iota(jnp.int32, (2 * n_rows, dim), 0) % 2
        out = None
        for k in range(2):
            hid = dot(ins, win_v[k], 1, 0)
            hid = (0.5 * hid * (1.0 + lax.erf(hid * 0.7071067811865476))).astype(BF16)
            res = dot(hid, wout_v[k], 1, 0)
            out = res if out is None else jnp.where(parity == k, res, out)
        part_v[...] = out.reshape(2, n_rows, dim)

    with scope("out_exchange"):
        part_copy = to_partner(part_v.at[other], peer_v, 4)
        part_copy.start()
        part_copy.wait()

    with scope("send2"):
        ys_v[...] = (part_v[core] + peer_v[...]).astype(BF16)
        ag_v[chip] = ys_v[...]
        for to in peers:
            pltpu.make_async_remote_copy(ys_v, ag_v.at[chip], sems.at[6], sems.at[7], device_id={"seq": to}, device_id_type=MESH).start()

    with scope("mix2"):
        @pl.loop(half, n_batch)
        def _(q):
            x_copy(q).wait()
            mix_weights(q)

    with scope("wait_ag"):
        arrived = ag_v.at[pl.ds(1, chips - 1)]
        pltpu.make_async_copy(arrived, arrived, sems.at[7]).wait()

    with scope("unpack"):
        for d in range(dim // 128):
            cols = slice(d * 128, (d + 1) * 128)
            unpack_v[d] = ag_v[:, :, cols].astype(F32).reshape(chips * n_rows, 128)
            for i in range(half):
                for k in range(2):
                    slots_v[first + i, k * chips:(k + 1) * chips, cols] = unpack_v[d, pl.ds(2 * i + k, chips, stride=n_rows), :].astype(BF16)

    with scope("finish"):
        mine = slots_v.at[pl.ds(first, half)]
        give = to_partner(mine, mine, 8)
        give.start()
        sent = send_v.at[pl.ds(1, chips - 1)]
        pltpu.make_async_copy(sent, sent, sems.at[0]).wait()
        sent = ag_v.at[pl.ds(1, chips - 1)]
        pltpu.make_async_copy(sent, sent, sems.at[6]).wait()
        give.wait()


def mix_kernel(left, c, slots, y_hbm, y_v, sem):
    n_batch, toks, _ = c.shape
    rows, parts = 256, 2

    def put(b, h):
        span = pl.ds(h * (toks // parts), toks // parts)
        return pltpu.make_async_copy(y_v.at[b, span], y_hbm.at[b, span], sem)

    @pl.loop(0, n_batch)
    def _(b):
        bound = jnp.broadcast_to(left[pl.ds(b, 1), :1], (rows, slots.shape[2]))
        for h in range(parts):
            for t in range(h * (toks // parts), (h + 1) * (toks // parts), rows):
                span = slice(t, t + rows)
                out = dot(c[b, span, :], slots[b], 1, 0)
                pos = lax.broadcasted_iota(jnp.int32, out.shape, 0) + t
                y_v[b, span, :] = jnp.where(pos < bound, out, 0.0).astype(BF16)
            put(b, h).start()

    pltpu.make_async_copy(y_v, y_hbm, sem).wait()


def solution(mesh):
    def local_layer(tokens, lengths, slot_params, logit_scale, w_in, w_out):
        n_batch, toks, dim = tokens.shape
        slots = slot_params.shape[1]
        chips, half = slots // 2, n_batch // 2
        n_rows = 2 * half
        vmem = pl.BlockSpec(memory_space=pltpu.VMEM)
        hbm = pl.BlockSpec(memory_space=pltpu.HBM)
        dma = pltpu.SemaphoreType.DMA
        weights, slot_out, left = pl.pallas_call(
            moe_kernel,
            name="moe",
            out_shape=(pltpu.VMEM((n_batch, toks, slots), BF16), pltpu.VMEM((n_batch, slots, dim), BF16), pltpu.VMEM((n_batch, 128), jnp.int32)),
            in_specs=[hbm, pl.BlockSpec(memory_space=pltpu.SMEM)] + [hbm] * 4,
            out_specs=(vmem, vmem, vmem),
            scratch_shapes=[
                pltpu.SMEM((n_batch,), jnp.int32),
                                pltpu.VMEM(slot_params.shape, BF16),
                pltpu.VMEM((n_batch, toks, dim), BF16),
                pltpu.VMEM(w_in.shape, BF16),
                pltpu.VMEM(w_out.shape, BF16),
                pltpu.VMEM((toks, dim), BF16),
                pltpu.VMEM((dim, slots), BF16),
                pltpu.VMEM((slots, dim), BF16),
                pltpu.VMEM((dim // 128, slots, 128), F32),
                pltpu.VMEM((slots, toks), F32),
                pltpu.VMEM((slots, toks), BF16),
                pltpu.VMEM((dim // 128 + 1, chips * n_rows, 128), F32),
                pltpu.VMEM((chips, n_rows, dim + 128), BF16),
                pltpu.VMEM((chips, n_rows, dim + 128), BF16),
                pltpu.VMEM((2, n_rows, dim), BF16),
                pltpu.VMEM((2, n_rows, dim), F32),
                pltpu.VMEM((n_rows, dim), F32),
                pltpu.VMEM((n_rows, dim), BF16),
                pltpu.VMEM((chips, n_rows, dim), BF16),
                pltpu.VMEM((dim // 128, chips * n_rows, 128), F32),
                dma((n_batch,)), dma((5,)), dma((10,)),
            ],
            compiler_params=pltpu.CompilerParams(collective_id=0, has_side_effects=True, vmem_limit_bytes=63100000),
        )(lengths, logit_scale, slot_params, tokens, w_in, w_out)
        return pl.pallas_call(
            mix_kernel,
            name="mix",
            out_shape=jax.ShapeDtypeStruct(tokens.shape, BF16),
            in_specs=[vmem, vmem, vmem],
            out_specs=hbm,
            scratch_shapes=[pltpu.VMEM(tokens.shape, BF16), dma],
            compiler_params=pltpu.CompilerParams(vmem_limit_bytes=20 * 2**20),
        )(left, weights, slot_out)

    return jax.shard_map(local_layer, mesh=mesh, in_specs=(P("data", "seq", None), P("data"), P(), P(), P("seq", None, "model"), P("seq", "model", None)), out_specs=P("data", "seq", None), check_vma=False)
```

```python
import jax
import jax.numpy as jnp
from jax import lax
from jax.experimental import pallas as pl
from jax.experimental.pallas import tpu as pltpu
from jax.sharding import PartitionSpec as P

NORM_EPS = 1e-6
MESH = pl.DeviceIdType.MESH
SIDE = 4
F32, BF16 = jnp.float32, jnp.bfloat16
NEG = -1e30
LOG2E = 1.4426950408889634
ROUNDS = 2
scope = jax.named_scope


def dot(a, b, ca, cb):
    return lax.dot_general(a, b, (((ca,), (cb,)), ((), ())), preferred_element_type=F32)


def far_first():
    near = (0, 1, 2, 1)
    every = [(z, y, x) for z in range(SIDE) for y in range(SIDE) for x in range(SIDE)]
    return sorted(every[1:], key=lambda o: (-sum(near[i] for i in o), o))


def mix_rows(c, slots, left, b, at, span):
    outs = jnp.concatenate([slots[0, at], slots[1, at]], axis=0)
    out = dot(c[b, span, :], outs, 1, 0)
    pos = lax.broadcasted_iota(jnp.int32, out.shape, 0) + span.start
    bound = jnp.broadcast_to(left[pl.ds(b, 1), :1], out.shape)
    return jnp.where(pos < bound, out, 0.0).astype(BF16)


def moe_kernel(lens_hbm, scale, phi_hbm, x_hbm, win_hbm, wout_hbm, c_v, slots_v, left_v, y_v,
               lens, phi, x_v, win_v, wout_v, u_v, v_v, vt_v, tmp_v, lt_v, w_v, pack_v, send_v, recv_v,
               xs_v, xin_v, xout_v, ys_v, ag_v, unpack_v,
               x_sem, l_sem, sems):
    n_batch, toks, dim = x_hbm.shape
    half = n_batch // 2
    per = half // ROUNDS
    slots = phi.shape[1]
    chips = slots // 2
    n_rows = 2 * per
    core = lax.axis_index("model")
    chip = lax.axis_index("seq")
    cz, cy, cx = chip // (SIDE * SIDE), (chip // SIDE) % SIDE, chip % SIDE
    first = core * half
    other = 1 - core

    def batch_of(q):
        return lax.rem(first + q, n_batch)

    def x_copy(q):
        return pltpu.make_async_copy(x_hbm.at[batch_of(q)], x_v.at[q], x_sem.at[q])

    loads = [pltpu.make_async_copy(a, b, l_sem.at[i]) for i, (a, b) in enumerate(
        ((phi_hbm, phi), (lens_hbm, lens), (win_hbm.at[core], win_v.at[core]), (wout_hbm.at[core], wout_v.at[core])))]

    def to_partner(src, dst, i, h):
        return pltpu.make_async_remote_copy(src, dst, sems.at[i, h], sems.at[i + 1, h], device_id={"model": other}, device_id_type=MESH)

    swaps = [to_partner(win_hbm.at[other], win_v.at[core], 4, 0), to_partner(wout_hbm.at[other], wout_v.at[core], 4, 1)]

    late = 8 * cz + 5 * cy + 4 * cx
    early = jnp.where(late <= 20, 1, 0)
    sums_first = per + (half - per) * early
    mix_first = early * jnp.where(late <= 4, 2, jnp.where(late <= 14, 1, 0))
    mix_between = mix_first + 2 * early
    mix_next = 3 + 4 * early
    for load in loads[:2]:
        load.start()
    for q in range(per):
        x_copy(q).start()

    at_z = [(cz + d) % SIDE * (SIDE * SIDE) for d in range(SIDE)]
    at_y = [(cy + d) % SIDE * SIDE for d in range(SIDE)]
    at_x = [(cx + d) % SIDE for d in range(SIDE)]
    peers = [at_z[z] + at_y[y] + at_x[x] for z, y, x in far_first()]

    with scope("signal"):
        barrier = pltpu.get_barrier_semaphore()
        for to in peers:
            pl.semaphore_signal(barrier, inc=1, device_id={"seq": to}, device_id_type=MESH)
        pl.semaphore_signal(barrier, inc=1, device_id={"model": other}, device_id_type=MESH)

    with scope("phi"):
        for load in loads[:2]:
            load.wait()
        for q in range(per, n_batch):
            x_copy(q).start()
        for load in loads[2:]:
            load.start()
        g = scale[...] * LOG2E
        p32 = phi[...].astype(F32)
        unit = (p32 * lax.rsqrt(jnp.sum(p32 * p32, axis=0, keepdims=True) + NORM_EPS))
        for d in range(dim // 128):
            cols = slice(d * 128, (d + 1) * 128)
            tmp_v[d] = unit[cols, :].T
            for k in range(2):
                vt_v[k * chips:(k + 1) * chips, cols] = tmp_v[d, pl.ds(k, chips, stride=2), :].astype(BF16)
        v_v[...] = vt_v[...].astype(F32).T.astype(BF16)
        for b in range(n_batch):
            left_v[b:b + 1, :] = jnp.full((1, 128), lens[b] - chip * toks, jnp.int32)

    def unit_rows(q, u, start, size):
        for t in range(start, start + size, 64):
            span = slice(t, t + 64)
            part = x_v[q, span, :].astype(F32)
            norm = lax.rsqrt(jnp.sum(part * part, axis=1, keepdims=True) + NORM_EPS)
            u[span, :] = (x_v[q, span, :].astype(F32) * norm).astype(BF16)

    rows = 256
    lane = lax.broadcasted_iota(jnp.int32, (slots, 128), 1)
    spans = [slice(t, t + rows) for t in range(0, toks, rows)]

    def dispatch(q):
        x_copy(q).wait()
        u, lt, w_b = u_v, lt_v, w_v
        h, i = q // per, q % per
        left = lens[batch_of(q)] - chip * toks
        bias = jnp.where(lax.broadcasted_iota(jnp.int32, (1, toks), 1) < left, 0.0, NEG)
        top = jnp.full((slots, rows), NEG, F32)
        for span in spans:
            unit_rows(q, u, span.start, rows)
            lg = g * dot(vt_v[...], u[span, :], 1, 1) + bias[:, span]
            lt[:, span] = lg
            top = jnp.maximum(top, lg)
        top = jnp.max(top, axis=1, keepdims=True)
        total = jnp.zeros((slots, rows), F32)
        for span in spans:
            w = jnp.exp2(lt[:, span] - top)
            total = total + w
            w_b[:, span] = w.astype(BF16)
        total = jnp.sum(total, axis=1, keepdims=True)
        sums = dot(w_b[...], x_v[q], 1, 0)
        stat = jnp.zeros((slots, 128), F32)
        for pos, val in ((0, top), (3, total)):
            rest = val
            for j in range(3):
                piece = rest.astype(BF16).astype(F32)
                rest = rest - piece
                stat = jnp.where(lane == pos + j, piece, stat)
        for k in range(2):
            dst = pl.ds(k * per + i, chips, stride=n_rows)
            for d in range(dim // 128):
                pack_v[h, d, dst, :] = sums[k * chips:(k + 1) * chips, d * 128:(d + 1) * 128]
            pack_v[h, dim // 128, dst, :] = stat[k * chips:(k + 1) * chips, :]

    def send_sums(h):
        for d in range(dim // 128 + 1):
            send_v[h, :, :, d * 128:(d + 1) * 128] = pack_v[h, d].astype(BF16).reshape(chips, n_rows, 128)
        recv_v[h, chip] = send_v[h, chip]
        for to in peers:
            pltpu.make_async_remote_copy(send_v.at[h, to], recv_v.at[h, chip], sems.at[0, h], sems.at[1, h], device_id={"seq": to}, device_id_type=MESH).start()

    def mix_weights(q):
        b = batch_of(q)
        for span in spans:
            unit_rows(q, u_v, span.start, rows)
            lg = g * dot(u_v[span, :], v_v[...], 1, 0)
            e = jnp.exp2(lg - jnp.max(lg, axis=1, keepdims=True))
            c_v[b, span, :] = (e / jnp.sum(e, axis=1, keepdims=True)).astype(BF16)

    def mix_span(name, lo, hi):
        with scope(name):
            @pl.loop(lo, hi)
            def _(q):
                mix_weights(q)

    with scope("dispatch"):
        @pl.loop(0, sums_first)
        def _(q):
            dispatch(q)
    mix_span("mix0", 0, mix_first)
    with scope("barrier"):
        pl.semaphore_wait(barrier, chips)
    with scope("send"):
        send_sums(0)
        for swap in swaps:
            swap.start()
    with scope("dispatch2"):
        @pl.loop(sums_first, half)
        def _(q):
            dispatch(q)
    mix_span("mix01", mix_first, mix_between)
    with scope("sendb"):
        send_sums(1)
    for q in range(half, n_batch):
        x_copy(q).wait()
    mix_span("mix1", mix_between, mix_next)

    def wait_bytes(ref, sem):
        pltpu.make_async_copy(ref, ref, sem).wait()

    sel_row = lax.broadcasted_iota(jnp.int32, (128, 128), 0)
    pick_top = (sel_row < 3).astype(F32).astype(BF16)
    pick_total = ((sel_row >= 3) & (sel_row < 6)).astype(F32).astype(BF16)

    for h in range(ROUNDS):
        with scope("wait_a2a"):
            wait_bytes(recv_v.at[h, pl.ds(1, chips - 1)], sems.at[1, h])
        with scope("meet"):
            got = recv_v[h, :, :, dim:].astype(F32).reshape(chips * n_rows, 128).astype(BF16)
            tops = dot(got, pick_top, 1, 0).reshape(chips, n_rows, 128)
            totals = dot(got, pick_total, 1, 0).reshape(chips, n_rows, 128)
            factor = jnp.exp2(tops - jnp.max(tops, axis=0, keepdims=True))
            z = jnp.sum(factor * totals, axis=0)
            for d in range(dim // 128):
                cols = slice(d * 128, (d + 1) * 128)
                acc = jnp.sum(factor * recv_v[h, :, :, cols].astype(F32), axis=0)
                xs_v[:, :, cols] = (acc / z).reshape(2, per, 128)
            xin_v[h, core] = xs_v[core].astype(BF16)
            xout_v[h] = xs_v[other].astype(BF16)
        with scope("xs_exchange"):
            xs_copy = to_partner(xout_v.at[h], xin_v.at[h, core], 2, h)
            xs_copy.start()
            if h == 0:
                for load in loads[2:] + swaps:
                    load.wait()
            xs_copy.wait()
        with scope("ffn"):
            ins = xin_v[h].astype(F32).reshape(n_rows, dim).astype(BF16)
            out = 0.0
            for m in range(2):
                hid = dot(ins, win_v[m], 1, 0)
                hid = (0.5 * hid * (1.0 + lax.erf(hid * 0.7071067811865476))).astype(BF16)
                out = out + dot(hid, wout_v[m], 1, 0)
            ys_v[h] = out.astype(BF16)
            ag_v[h, chip] = ys_v[h]
        with scope("send2"):
            for to in peers:
                pltpu.make_async_remote_copy(ys_v.at[h], ag_v.at[h, chip], sems.at[6, h], sems.at[7, h], device_id={"seq": to}, device_id_type=MESH).start()

    mix_span("mix2", mix_next, n_batch)

    gives = []

    def unpack(h):
        with scope("wait_ag"):
            wait_bytes(ag_v.at[h, pl.ds(1, chips - 1)], sems.at[7, h])
        with scope("unpack"):
            for d in range(dim // 128):
                cols = slice(d * 128, (d + 1) * 128)
                unpack_v[d] = ag_v[h, :, :, cols].astype(F32).reshape(chips * n_rows, 128)
                for r in range(n_rows):
                    slots_v[core, h * n_rows + r, :, cols] = unpack_v[d, pl.ds(r, chips, stride=n_rows), :].astype(BF16)
            mine = slots_v.at[core, pl.ds(h * n_rows, n_rows)]
            give = to_partner(mine, mine, 8, h)
            give.start()
            gives.append(give)

    def mix_early(lo, hi):
        with scope("mix_early"):
            @pl.loop(lo, hi)
            def _(j):
                for span in spans:
                    y_v[j, span, :] = mix_rows(c_v, slots_v, left_v, j // per * half + j % per, j, span)

    unpack(0)
    with scope("wait_give"):
        gives[0].wait()
    mix_early(0, n_rows // 2)
    unpack(1)
    mix_early(n_rows // 2, n_rows)

    with scope("finish"):
        for h in range(ROUNDS):
            wait_bytes(send_v.at[h, pl.ds(1, chips - 1)], sems.at[0, h])
            wait_bytes(ag_v.at[h, pl.ds(1, chips - 1)], sems.at[6, h])
        gives[1].wait()


def mix_kernel(left, c, slots, y_v, y_hbm, rest_v, sems):
    n_batch, toks, _ = c.shape
    done, half = y_v.shape[0], n_batch // 2
    per = half // ROUNDS
    rows, parts = 256, 2

    def batch_of(j, h):
        return j // per * half + h * per + j % per

    for j in range(done):
        pltpu.make_async_copy(y_v.at[j], y_hbm.at[batch_of(j, 0)], sems.at[0]).start()

    @pl.loop(0, done)
    def _(j):
        b = batch_of(j, 1)
        for p in range(parts):
            for t in range(p * (toks // parts), (p + 1) * (toks // parts), rows):
                span = slice(t, t + rows)
                rest_v[j, span, :] = mix_rows(c, slots, left, b, done + j, span)
            span = pl.ds(p * (toks // parts), toks // parts)
            pltpu.make_async_copy(rest_v.at[j, span], y_hbm.at[b, span], sems.at[1]).start()

    pltpu.make_async_copy(y_v, y_hbm.at[pl.ds(0, done)], sems.at[0]).wait()
    pltpu.make_async_copy(rest_v, y_hbm.at[pl.ds(0, done)], sems.at[1]).wait()


def solution(mesh):
    def local_layer(tokens, lengths, slot_params, logit_scale, w_in, w_out):
        n_batch, toks, dim = tokens.shape
        slots = slot_params.shape[1]
        chips, half = slots // 2, n_batch // 2
        per = half // ROUNDS
        n_rows = 2 * per
        vmem = pl.BlockSpec(memory_space=pltpu.VMEM)
        hbm = pl.BlockSpec(memory_space=pltpu.HBM)
        dma = pltpu.SemaphoreType.DMA
        weights, slot_out, left, mixed = pl.pallas_call(
            moe_kernel,
            name="moe",
            out_shape=(pltpu.VMEM((n_batch, toks, slots), BF16), pltpu.VMEM((2, n_batch, chips, dim), BF16), pltpu.VMEM((n_batch, 128), jnp.int32), pltpu.VMEM((half, toks, dim), BF16)),
            in_specs=[hbm, pl.BlockSpec(memory_space=pltpu.SMEM)] + [hbm] * 4,
            out_specs=(vmem, vmem, vmem, vmem),
            scratch_shapes=[
                pltpu.SMEM((n_batch,), jnp.int32),
                pltpu.VMEM(slot_params.shape, BF16),
                pltpu.VMEM((n_batch, toks, dim), BF16),
                pltpu.VMEM(w_in.shape, BF16),
                pltpu.VMEM(w_out.shape, BF16),
                pltpu.VMEM((toks, dim), BF16),
                pltpu.VMEM((dim, slots), BF16),
                pltpu.VMEM((slots, dim), BF16),
                pltpu.VMEM((dim // 128, slots, 128), F32),
                pltpu.VMEM((slots, toks), F32),
                pltpu.VMEM((slots, toks), BF16),
                pltpu.VMEM((ROUNDS, dim // 128 + 1, chips * n_rows, 128), F32),
                pltpu.VMEM((ROUNDS, chips, n_rows, dim + 128), BF16),
                pltpu.VMEM((ROUNDS, chips, n_rows, dim + 128), BF16),
                pltpu.VMEM((2, per, dim), F32),
                pltpu.VMEM((ROUNDS, 2, per, dim), BF16),
                pltpu.VMEM((ROUNDS, per, dim), BF16),
                pltpu.VMEM((ROUNDS, n_rows, dim), BF16),
                pltpu.VMEM((ROUNDS, chips, n_rows, dim), BF16),
                pltpu.VMEM((dim // 128, chips * n_rows, 128), F32),
                dma((n_batch,)), dma((4,)), dma((10, ROUNDS)),
            ],
            compiler_params=pltpu.CompilerParams(collective_id=0, has_side_effects=True, vmem_limit_bytes=58380000),
        )(lengths, logit_scale, slot_params, tokens, w_in, w_out)
        return pl.pallas_call(
            mix_kernel,
            name="mix",
            out_shape=jax.ShapeDtypeStruct(tokens.shape, BF16),
            in_specs=[vmem, vmem, vmem, vmem],
            out_specs=hbm,
            scratch_shapes=[pltpu.VMEM((half, toks, dim), BF16), dma((2,))],
            compiler_params=pltpu.CompilerParams(vmem_limit_bytes=20 * 2**20),
        )(left, weights, slot_out, mixed)

    return jax.shard_map(local_layer, mesh=mesh, in_specs=(P("data", "seq", None), P("data"), P(), P(), P("seq", None, "model"), P("seq", "model", None)), out_specs=P("data", "seq", None), check_vma=False)
```

```python
import jax
import jax.numpy as jnp
from jax import lax
from jax.experimental import pallas as pl
from jax.experimental.pallas import tpu as pltpu
from jax.sharding import PartitionSpec as P

NORM_EPS = 1e-6
MESH = pl.DeviceIdType.MESH
SIDE = 4
F32, BF16 = jnp.float32, jnp.bfloat16
NEG = -1e30
LOG2E = 1.4426950408889634
ROUNDS = 2
DIRECT = (0, 1, 4)
scope = jax.named_scope


def dot(a, b, ca, cb):
    return lax.dot_general(a, b, (((ca,), (cb,)), ((), ())), preferred_element_type=F32)


def far_first():
    near = (0, 1, 2, 1)
    every = [(z, y, x) for z in range(SIDE) for y in range(SIDE) for x in range(SIDE)]
    return sorted(every[1:], key=lambda o: (-sum(near[i] for i in o), o))


def mix_rows(c, slots, left, b, at, span):
    outs = jnp.concatenate([slots[0, at], slots[1, at]], axis=0)
    out = dot(c[b, span, :], outs, 1, 0)
    pos = lax.broadcasted_iota(jnp.int32, out.shape, 0) + span.start
    bound = jnp.broadcast_to(left[pl.ds(b, 1), :1], out.shape)
    return jnp.where(pos < bound, out, 0.0).astype(BF16)


def moe_kernel(lens_hbm, scale, phi_hbm, x_hbm, win_hbm, wout_hbm, c_v, slots_v, left_v, y_v,
               lens, phi, x_v, win_v, wout_v, u_v, v_v, vt_v, tmp_v, lt_v, w_v, pack_v, send_v, recv_v,
               xs_v, xin_v, xout_v, ys_v, ag_v, agx_v, unpack_v,
               x_sem, l_sem, sems):
    n_batch, toks, dim = x_hbm.shape
    half = n_batch // 2
    per = half // ROUNDS
    slots = phi.shape[1]
    chips = slots // 2
    n_rows = 2 * per
    core = lax.axis_index("model")
    chip = lax.axis_index("seq")
    cz, cy, cx = chip // (SIDE * SIDE), (chip // SIDE) % SIDE, chip % SIDE
    first = core * half
    other = 1 - core

    def batch_of(q):
        return lax.rem(first + q, n_batch)

    def x_copy(q):
        return pltpu.make_async_copy(x_hbm.at[batch_of(q)], x_v.at[q], x_sem.at[q])

    loads = [pltpu.make_async_copy(a, b, l_sem.at[i]) for i, (a, b) in enumerate(
        ((phi_hbm, phi), (lens_hbm, lens), (win_hbm.at[core], win_v.at[core]), (wout_hbm.at[core], wout_v.at[core])))]

    def to_partner(src, dst, i, h):
        return pltpu.make_async_remote_copy(src, dst, sems.at[i, h], sems.at[i + 1, h], device_id={"model": other}, device_id_type=MESH)

    swaps = [to_partner(win_hbm.at[other], win_v.at[core], 4, 0), to_partner(wout_hbm.at[other], wout_v.at[core], 4, 1)]

    late = 8 * cz + 5 * cy + 4 * cx
    early = jnp.where(late <= 20, 1, 0)
    sums_first = per + (half - per) * early
    mix_first = early * jnp.where(late <= 4, 2, jnp.where(late <= 14, 1, 0))
    mix_between = mix_first + 2 * early
    mix_next = jnp.where(early == 1, mix_between + 2, 3)
    for load in loads[:2]:
        load.start()
    for q in range(per):
        x_copy(q).start()

    at_z = [(cz + d) % SIDE * (SIDE * SIDE) for d in range(SIDE)]
    at_y = [(cy + d) % SIDE * SIDE for d in range(SIDE)]
    at_x = [(cx + d) % SIDE for d in range(SIDE)]
    peers = [at_z[z] + at_y[y] + at_x[x] for z, y, x in far_first()]

    in_direct = sum((chip == e).astype(jnp.int32) for e in DIRECT)
    gets_both = in_direct == 1

    by_start = sorted(range(chips), key=lambda a: 8 * (a // 16) + 5 * (a // 4 % 4) + 4 * (a % 4))
    with scope("signal"):
        barrier = pltpu.get_barrier_semaphore()
        for to in [jnp.where(chip == a, by_start[-1], a) for a in by_start[:-1]]:
            pl.semaphore_signal(barrier, inc=1, device_id={"seq": to}, device_id_type=MESH)
        pl.semaphore_signal(barrier, inc=1, device_id={"model": other}, device_id_type=MESH)

        @pl.when(gets_both)
        def _():
            for to in peers:
                pl.semaphore_signal(barrier, inc=1, device_id={"model": other, "seq": to}, device_id_type=MESH)

    with scope("phi"):
        for load in loads[:2]:
            load.wait()
        for q in range(per, n_batch):
            x_copy(q).start()
        for load in loads[2:]:
            load.start()
        g = scale[...] * LOG2E
        p32 = phi[...].astype(F32)
        unit = (p32 * lax.rsqrt(jnp.sum(p32 * p32, axis=0, keepdims=True) + NORM_EPS))
        for d in range(dim // 128):
            cols = slice(d * 128, (d + 1) * 128)
            tmp_v[d] = unit[cols, :].T
            for k in range(2):
                vt_v[k * chips:(k + 1) * chips, cols] = tmp_v[d, pl.ds(k, chips, stride=2), :].astype(BF16)
        v_v[...] = vt_v[...].astype(F32).T.astype(BF16)
        for b in range(n_batch):
            left_v[b:b + 1, :] = jnp.full((1, 128), lens[b] - chip * toks, jnp.int32)

    def unit_rows(q, u, start, size):
        for t in range(start, start + size, 64):
            span = slice(t, t + 64)
            part = x_v[q, span, :].astype(F32)
            norm = lax.rsqrt(jnp.sum(part * part, axis=1, keepdims=True) + NORM_EPS)
            u[span, :] = (x_v[q, span, :].astype(F32) * norm).astype(BF16)

    rows = 256
    lane = lax.broadcasted_iota(jnp.int32, (slots, 128), 1)
    spans = [slice(t, t + rows) for t in range(0, toks, rows)]

    def dispatch(q):
        x_copy(q).wait()
        u, lt, w_b = u_v, lt_v, w_v
        h, i = q // per, q % per
        left = lens[batch_of(q)] - chip * toks
        bias = jnp.where(lax.broadcasted_iota(jnp.int32, (1, toks), 1) < left, 0.0, NEG)
        top = jnp.full((slots, rows), NEG, F32)
        for span in spans:
            unit_rows(q, u, span.start, rows)
            lg = g * dot(vt_v[...], u[span, :], 1, 1) + bias[:, span]
            lt[:, span] = lg
            top = jnp.maximum(top, lg)
        top = jnp.max(top, axis=1, keepdims=True)
        total = jnp.zeros((slots, rows), F32)
        for span in spans:
            w = jnp.exp2(lt[:, span] - top)
            total = total + w
            w_b[:, span] = w.astype(BF16)
        total = jnp.sum(total, axis=1, keepdims=True)
        sums = dot(w_b[...], x_v[q], 1, 0)
        stat = jnp.zeros((slots, 128), F32)
        for pos, val in ((0, top), (3, total)):
            rest = val
            for j in range(3):
                piece = rest.astype(BF16).astype(F32)
                rest = rest - piece
                stat = jnp.where(lane == pos + j, piece, stat)
        for k in range(2):
            dst = pl.ds(k * per + i, chips, stride=n_rows)
            for d in range(dim // 128):
                pack_v[h, d, dst, :] = sums[k * chips:(k + 1) * chips, d * 128:(d + 1) * 128]
            pack_v[h, dim // 128, dst, :] = stat[k * chips:(k + 1) * chips, :]

    def serve_first(which):
        return [jnp.where(chip == which, peers[-1], which)] + [jnp.where(to == which, peers[-1], to) for to in peers[:-1]]

    def send_sums(h):
        for d in range(dim // 128 + 1):
            send_v[h, :, :, d * 128:(d + 1) * 128] = pack_v[h, d].astype(BF16).reshape(chips, n_rows, 128)
        recv_v[h, chip] = send_v[h, chip]
        for to in serve_first(chips - 1):
            pltpu.make_async_remote_copy(send_v.at[h, to], recv_v.at[h, chip], sems.at[0, h], sems.at[1, h], device_id={"seq": to}, device_id_type=MESH).start()

    def mix_weights(q):
        b = batch_of(q)
        for span in spans:
            unit_rows(q, u_v, span.start, rows)
            lg = g * dot(u_v[span, :], v_v[...], 1, 0)
            e = jnp.exp2(lg - jnp.max(lg, axis=1, keepdims=True))
            c_v[b, span, :] = (e / jnp.sum(e, axis=1, keepdims=True)).astype(BF16)

    def mix_span(name, lo, hi):
        with scope(name):
            @pl.loop(lo, hi)
            def _(q):
                mix_weights(q)

    with scope("dispatch"):
        @pl.loop(0, sums_first)
        def _(q):
            dispatch(q)
    mix_span("mix0", 0, mix_first)
    with scope("barrier"):
        pl.semaphore_wait(barrier, chips + len(DIRECT) - in_direct)
    with scope("send"):
        send_sums(0)
        for swap in swaps:
            swap.start()
    with scope("dispatch2"):
        @pl.loop(sums_first, half)
        def _(q):
            dispatch(q)
    mix_span("mix01", mix_first, mix_between)
    with scope("sendb"):
        send_sums(1)
    for q in range(half, n_batch):
        x_copy(q).wait()
    mix_span("mix1", mix_between, mix_next)

    def wait_bytes(ref, sem):
        pltpu.make_async_copy(ref, ref, sem).wait()

    sel_row = lax.broadcasted_iota(jnp.int32, (128, 128), 0)
    pick_top = (sel_row < 3).astype(F32).astype(BF16)
    pick_total = ((sel_row >= 3) & (sel_row < 6)).astype(F32).astype(BF16)

    for h in range(ROUNDS):
        with scope("wait_a2a"):
            wait_bytes(recv_v.at[h, pl.ds(1, chips - 1)], sems.at[1, h])
        with scope("meet"):
            got = recv_v[h, :, :, dim:].astype(F32).reshape(chips * n_rows, 128).astype(BF16)
            tops = dot(got, pick_top, 1, 0).reshape(chips, n_rows, 128)
            totals = dot(got, pick_total, 1, 0).reshape(chips, n_rows, 128)
            factor = jnp.exp2(tops - jnp.max(tops, axis=0, keepdims=True))
            z = jnp.sum(factor * totals, axis=0)
            for d in range(dim // 128):
                cols = slice(d * 128, (d + 1) * 128)
                acc = jnp.sum(factor * recv_v[h, :, :, cols].astype(F32), axis=0)
                xs_v[:, :, cols] = (acc / z).reshape(2, per, 128)
            xin_v[h, core] = xs_v[core].astype(BF16)
            xout_v[h] = xs_v[other].astype(BF16)
        with scope("xs_exchange"):
            xs_copy = to_partner(xout_v.at[h], xin_v.at[h, core], 2, h)
            xs_copy.start()
            if h == 0:
                for load in loads[2:] + swaps:
                    load.wait()
            xs_copy.wait()
        with scope("ffn"):
            ins = xin_v[h].astype(F32).reshape(n_rows, dim).astype(BF16)
            out = 0.0
            for m in range(2):
                hid = dot(ins, win_v[m], 1, 0)
                hid = (0.5 * hid * (1.0 + lax.erf(hid * 0.7071067811865476))).astype(BF16)
                out = out + dot(hid, wout_v[m], 1, 0)
            ys_v[h] = out.astype(BF16)
            ag_v[h, chip] = ys_v[h]
        with scope("send2"):
            for e in DIRECT:
                pltpu.make_async_remote_copy(ys_v.at[h], agx_v.at[h, chip], sems.at[10, h], sems.at[11, h], device_id={"model": other, "seq": e}, device_id_type=MESH).start()
            for to in serve_first(0):
                pltpu.make_async_remote_copy(ys_v.at[h], ag_v.at[h, chip], sems.at[6, h], sems.at[7, h], device_id={"seq": to}, device_id_type=MESH).start()

    mix_span("mix2", mix_next, n_batch)

    gives = []

    def spread(src, parity, h):
        for d in range(dim // 128):
            cols = slice(d * 128, (d + 1) * 128)
            unpack_v[d] = src[h, :, :, cols].astype(F32).reshape(chips * n_rows, 128)
            for r in range(n_rows):
                slots_v[parity, h * n_rows + r, :, cols] = unpack_v[d, pl.ds(r, chips, stride=n_rows), :].astype(BF16)

    def unpack(h):
        with scope("wait_ag"):
            wait_bytes(ag_v.at[h, pl.ds(1, chips - 1)], sems.at[7, h])
        with scope("unpack"):
            spread(ag_v, core, h)
            mine = slots_v.at[core, pl.ds(h * n_rows, n_rows)]
            give = to_partner(mine, mine, 8, h)
            gives.append(give)

            @pl.when(jnp.logical_not(gets_both))
            def _():
                give.start()

            @pl.when(gets_both)
            def _():
                wait_bytes(agx_v.at[h], sems.at[11, h])
                spread(agx_v, other, h)

    def settle(h):
        @pl.when(jnp.logical_not(gets_both))
        def _():
            gives[h].wait()

    def mix_early(lo, hi):
        with scope("mix_early"):
            @pl.loop(lo, hi)
            def _(j):
                for span in spans:
                    y_v[j, span, :] = mix_rows(c_v, slots_v, left_v, j // per * half + j % per, j, span)

    unpack(0)
    with scope("wait_give"):
        settle(0)
    early_rows = jnp.where(gets_both, n_rows, n_rows // 2)
    mix_early(0, early_rows)
    unpack(1)
    mix_early(early_rows, n_rows)

    with scope("finish"):
        for h in range(ROUNDS):
            wait_bytes(send_v.at[h, pl.ds(1, chips - 1)], sems.at[0, h])
            wait_bytes(ag_v.at[h, pl.ds(1, chips - 1)], sems.at[6, h])

            wait_bytes(agx_v.at[h, pl.ds(0, len(DIRECT))], sems.at[10, h])
        settle(1)


def mix_kernel(left, c, slots, y_v, y_hbm, rest_v, sems):
    n_batch, toks, _ = c.shape
    done, half = y_v.shape[0], n_batch // 2
    per = half // ROUNDS
    rows, parts = 256, 2

    def batch_of(j, h):
        return j // per * half + h * per + j % per

    for j in range(done):
        pltpu.make_async_copy(y_v.at[j], y_hbm.at[batch_of(j, 0)], sems.at[0]).start()

    @pl.loop(0, done)
    def _(j):
        b = batch_of(j, 1)
        for p in range(parts):
            for t in range(p * (toks // parts), (p + 1) * (toks // parts), rows):
                span = slice(t, t + rows)
                rest_v[j, span, :] = mix_rows(c, slots, left, b, done + j, span)
            span = pl.ds(p * (toks // parts), toks // parts)
            pltpu.make_async_copy(rest_v.at[j, span], y_hbm.at[b, span], sems.at[1]).start()

    pltpu.make_async_copy(y_v, y_hbm.at[pl.ds(0, done)], sems.at[0]).wait()
    pltpu.make_async_copy(rest_v, y_hbm.at[pl.ds(0, done)], sems.at[1]).wait()


def solution(mesh):
    def local_layer(tokens, lengths, slot_params, logit_scale, w_in, w_out):
        n_batch, toks, dim = tokens.shape
        slots = slot_params.shape[1]
        chips, half = slots // 2, n_batch // 2
        per = half // ROUNDS
        n_rows = 2 * per
        vmem = pl.BlockSpec(memory_space=pltpu.VMEM)
        hbm = pl.BlockSpec(memory_space=pltpu.HBM)
        dma = pltpu.SemaphoreType.DMA
        weights, slot_out, left, mixed = pl.pallas_call(
            moe_kernel,
            name="moe",
            out_shape=(pltpu.VMEM((n_batch, toks, slots), BF16), pltpu.VMEM((2, n_batch, chips, dim), BF16), pltpu.VMEM((n_batch, 128), jnp.int32), pltpu.VMEM((half, toks, dim), BF16)),
            in_specs=[hbm, pl.BlockSpec(memory_space=pltpu.SMEM)] + [hbm] * 4,
            out_specs=(vmem, vmem, vmem, vmem),
            scratch_shapes=[
                pltpu.SMEM((n_batch,), jnp.int32),
                pltpu.VMEM(slot_params.shape, BF16),
                pltpu.VMEM((n_batch, toks, dim), BF16),
                pltpu.VMEM(w_in.shape, BF16),
                pltpu.VMEM(w_out.shape, BF16),
                pltpu.VMEM((toks, dim), BF16),
                pltpu.VMEM((dim, slots), BF16),
                pltpu.VMEM((slots, dim), BF16),
                pltpu.VMEM((dim // 128, slots, 128), F32),
                pltpu.VMEM((slots, toks), F32),
                pltpu.VMEM((slots, toks), BF16),
                pltpu.VMEM((ROUNDS, dim // 128 + 1, chips * n_rows, 128), F32),
                pltpu.VMEM((ROUNDS, chips, n_rows, dim + 128), BF16),
                pltpu.VMEM((ROUNDS, chips, n_rows, dim + 128), BF16),
                pltpu.VMEM((2, per, dim), F32),
                pltpu.VMEM((ROUNDS, 2, per, dim), BF16),
                pltpu.VMEM((ROUNDS, per, dim), BF16),
                pltpu.VMEM((ROUNDS, n_rows, dim), BF16),
                pltpu.VMEM((ROUNDS, chips, n_rows, dim), BF16),
                pltpu.VMEM((ROUNDS, chips, n_rows, dim), BF16),
                pltpu.VMEM((dim // 128, chips * n_rows, 128), F32),
                dma((n_batch,)), dma((4,)), dma((12, ROUNDS)),
            ],
            compiler_params=pltpu.CompilerParams(collective_id=0, has_side_effects=True, vmem_limit_bytes=58380000),
        )(lengths, logit_scale, slot_params, tokens, w_in, w_out)
        return pl.pallas_call(
            mix_kernel,
            name="mix",
            out_shape=jax.ShapeDtypeStruct(tokens.shape, BF16),
            in_specs=[vmem, vmem, vmem, vmem],
            out_specs=hbm,
            scratch_shapes=[pltpu.VMEM((half, toks, dim), BF16), dma((2,))],
            compiler_params=pltpu.CompilerParams(vmem_limit_bytes=20 * 2**20),
        )(left, weights, slot_out, mixed)

    return jax.shard_map(local_layer, mesh=mesh, in_specs=(P("data", "seq", None), P("data"), P(), P(), P("seq", None, "model"), P("seq", "model", None)), out_specs=P("data", "seq", None), check_vma=False)
```

```python
import jax
import jax.numpy as jnp
from jax import lax
from jax.experimental import pallas as pl
from jax.experimental.pallas import tpu as pltpu
from jax.sharding import PartitionSpec as P

NORM_EPS = 1e-6
MESH = pl.DeviceIdType.MESH
SIDE = 4
F32, BF16 = jnp.float32, jnp.bfloat16
NEG = -1e30
LOG2E = 1.4426950408889634
ROUNDS = 2
DIRECT = (0, 1, 4)
scope = jax.named_scope


def dot(a, b, ca, cb):
    return lax.dot_general(a, b, (((ca,), (cb,)), ((), ())), preferred_element_type=F32)


def far_first():
    near = (0, 1, 2, 1)
    every = [(z, y, x) for z in range(SIDE) for y in range(SIDE) for x in range(SIDE)]
    return sorted(every[1:], key=lambda o: (-sum(near[i] for i in o), o))


def mix_rows(c, slots, left, b, at, span):
    outs = jnp.concatenate([slots[0, at], slots[1, at]], axis=0)
    out = dot(c[b, span, :], outs, 1, 0)
    pos = lax.broadcasted_iota(jnp.int32, out.shape, 0) + span.start
    bound = jnp.broadcast_to(left[pl.ds(b, 1), :1], out.shape)
    return jnp.where(pos < bound, out, 0.0).astype(BF16)


def moe_kernel(lens_hbm, scale, phi_hbm, x_hbm, win_hbm, wout_hbm, c_v, slots_v, left_v, y_v,
               lens, phi, x_v, win_v, wout_v, u_v, v_v, vt_v, tmp_v, lt_v, w_v, pack_v, send_v, recv_v,
               xs_v, xin_v, xout_v, ys_v, ag_v, agx_v, unpack_v,
               x_sem, l_sem, send_sem, recv_sem):
    n_batch, toks, dim = x_hbm.shape
    half = n_batch // 2
    per = half // ROUNDS
    slots = phi.shape[1]
    chips = slots // 2
    n_rows = 2 * per
    core = lax.axis_index("model")
    chip = lax.axis_index("seq")
    cz, cy, cx = chip // (SIDE * SIDE), (chip // SIDE) % SIDE, chip % SIDE
    first = core * half
    other = 1 - core

    def wait_bytes(ref, sem):
        pltpu.make_async_copy(ref, ref, sem).wait()

    def batch_of(q):
        return lax.rem(first + q, n_batch)

    def x_copy(q):
        return pltpu.make_async_copy(x_hbm.at[batch_of(q)], x_v.at[q], x_sem.at[0 if q == 0 else 1 if q < half else 2])

    loads = [pltpu.make_async_copy(a, b, l_sem.at[min(i, 2)]) for i, (a, b) in enumerate(
        ((phi_hbm, phi), (lens_hbm, lens), (win_hbm.at[core], win_v.at[core]), (wout_hbm.at[core], wout_v.at[core])))]

    def to_partner(src, dst, i, h):
        return pltpu.make_async_remote_copy(src, dst, send_sem.at[i], recv_sem.at[i, h], device_id={"model": other}, device_id_type=MESH)

    swaps = [to_partner(win_hbm.at[other], win_v.at[core], 5, 0), to_partner(wout_hbm.at[other], wout_v.at[core], 5, 0)]

    late = 8 * cz + 5 * cy + 4 * cx
    early = jnp.where(late <= 20, 1, 0)
    sums_first = per + (half - per) * early
    mix_first = early * jnp.where(late <= 4, 2, jnp.where(late <= 14, 1, 0))
    mix_between = mix_first + early * (2 - jnp.where(late <= 4, 1 - core, 0))
    mix_next = jnp.where(early == 1, mix_between + 2, 3)
    for load in loads[:2]:
        load.start()
    for q in range(per):
        x_copy(q).start()

    at_z = [(cz + d) % SIDE * (SIDE * SIDE) for d in range(SIDE)]
    at_y = [(cy + d) % SIDE * SIDE for d in range(SIDE)]
    at_x = [(cx + d) % SIDE for d in range(SIDE)]
    peers = [at_z[z] + at_y[y] + at_x[x] for z, y, x in far_first()]

    in_direct = sum((chip == e).astype(jnp.int32) for e in DIRECT)
    gets_both = in_direct == 1

    by_start = sorted(range(chips), key=lambda a: 8 * (a // 16) + 5 * (a // 4 % 4) + 4 * (a % 4))
    with scope("signal"):
        barrier = pltpu.get_barrier_semaphore()
        for to in [jnp.where(chip == a, by_start[-1], a) for a in by_start[:-1]]:
            pl.semaphore_signal(barrier, inc=1, device_id={"seq": to}, device_id_type=MESH)
        pl.semaphore_signal(barrier, inc=1, device_id={"model": other}, device_id_type=MESH)

        @pl.when(gets_both)
        def _():
            for to in peers:
                pl.semaphore_signal(barrier, inc=1, device_id={"model": other, "seq": to}, device_id_type=MESH)

    with scope("phi"):
        for load in loads[:2]:
            load.wait()
        for q in range(per, n_batch):
            x_copy(q).start()
        for load in loads[2:]:
            load.start()
        g = scale[...] * LOG2E
        p32 = phi[...].astype(F32)
        unit = (p32 * lax.rsqrt(jnp.sum(p32 * p32, axis=0, keepdims=True) + NORM_EPS))
        for d in range(dim // 128):
            cols = slice(d * 128, (d + 1) * 128)
            tmp_v[d] = unit[cols, :].T
            for k in range(2):
                vt_v[k * chips:(k + 1) * chips, cols] = tmp_v[d, pl.ds(k, chips, stride=2), :].astype(BF16)
        v_v[...] = vt_v[...].astype(F32).T.astype(BF16)
        for b in range(n_batch):
            left_v[b:b + 1, :] = jnp.full((1, 128), lens[b] - chip * toks, jnp.int32)

    def unit_rows(q, u, start, size):
        for t in range(start, start + size, 64):
            span = slice(t, t + 64)
            part = x_v[q, span, :].astype(F32)
            norm = lax.rsqrt(jnp.sum(part * part, axis=1, keepdims=True) + NORM_EPS)
            u[span, :] = (x_v[q, span, :].astype(F32) * norm).astype(BF16)

    rows = 256
    lane = lax.broadcasted_iota(jnp.int32, (slots, 128), 1)
    spans = [slice(t, t + rows) for t in range(0, toks, rows)]

    def dispatch(q):
        @pl.when(q == 1)
        def _():
            wait_bytes(x_v.at[pl.ds(1, half - 1)], x_sem.at[1])
        u, lt, w_b = u_v, lt_v, w_v
        h, i = q // per, q % per
        left = lens[batch_of(q)] - chip * toks
        bias = jnp.where(lax.broadcasted_iota(jnp.int32, (1, toks), 1) < left, 0.0, NEG)
        top = jnp.full((slots, rows), NEG, F32)
        for span in spans:
            unit_rows(q, u, span.start, rows)
            lg = g * dot(vt_v[...], u[span, :], 1, 1) + bias[:, span]
            lt[:, span] = lg
            top = jnp.maximum(top, lg)
        top = jnp.max(top, axis=1, keepdims=True)
        total = jnp.zeros((slots, rows), F32)
        for span in spans:
            w = jnp.exp2(lt[:, span] - top)
            total = total + w
            w_b[:, span] = w.astype(BF16)
        total = jnp.sum(total, axis=1, keepdims=True)
        sums = dot(w_b[...], x_v[q], 1, 0)
        stat = jnp.zeros((slots, 128), F32)
        for pos, val in ((0, top), (3, total)):
            rest = val
            for j in range(3):
                piece = rest.astype(BF16).astype(F32)
                rest = rest - piece
                stat = jnp.where(lane == pos + j, piece, stat)
        for k in range(2):
            dst = pl.ds(k * per + i, chips, stride=n_rows)
            for d in range(dim // 128):
                pack_v[h, d, dst, :] = sums[k * chips:(k + 1) * chips, d * 128:(d + 1) * 128]
            pack_v[h, dim // 128, dst, :] = stat[k * chips:(k + 1) * chips, :]

    def serve_first(*favoured):
        order = list(peers)
        for a in reversed(favoured):
            last = order[-1]
            order = [jnp.where(chip == a, last, a)] + [jnp.where(to == a, last, to) for to in order[:-1]]
        return order

    def send_sums(h):
        for d in range(dim // 128 + 1):
            send_v[h, :, :, d * 128:(d + 1) * 128] = pack_v[h, d].astype(BF16).reshape(chips, n_rows, 128)
        recv_v[h, chip] = send_v[h, chip]
        for to in serve_first(63):
            pltpu.make_async_remote_copy(send_v.at[h, to], recv_v.at[h, chip], send_sem.at[0], recv_sem.at[0, h], device_id={"seq": to}, device_id_type=MESH).start()

    def mix_weights(q):
        b = batch_of(q)
        for span in spans:
            unit_rows(q, u_v, span.start, rows)
            lg = g * dot(u_v[span, :], v_v[...], 1, 0)
            e = jnp.exp2(lg - jnp.max(lg, axis=1, keepdims=True))
            c_v[b, span, :] = (e / jnp.sum(e, axis=1, keepdims=True)).astype(BF16)

    def mix_span(name, lo, hi):
        with scope(name):
            @pl.loop(lo, hi)
            def _(q):
                mix_weights(q)

    with scope("dispatch"):
        wait_bytes(x_v.at[0], x_sem.at[0])

        @pl.loop(0, sums_first)
        def _(q):
            dispatch(q)
    mix_span("mix0", 0, mix_first)
    with scope("barrier"):
        pl.semaphore_wait(barrier, chips + len(DIRECT) - in_direct)
    with scope("send"):
        send_sums(0)
        for swap in swaps:
            swap.start()
    with scope("dispatch2"):
        @pl.loop(sums_first, half)
        def _(q):
            dispatch(q)
    mix_span("mix01", mix_first, mix_between)
    with scope("sendb"):
        send_sums(1)
    wait_bytes(x_v.at[pl.ds(half, n_batch - half)], x_sem.at[2])
    mix_span("mix1", mix_between, mix_next)

    sel_row = lax.broadcasted_iota(jnp.int32, (128, 128), 0)
    pick_top = (sel_row < 3).astype(F32).astype(BF16)
    pick_total = ((sel_row >= 3) & (sel_row < 6)).astype(F32).astype(BF16)

    for h in range(ROUNDS):
        with scope("wait_a2a"):
            wait_bytes(recv_v.at[h, pl.ds(1, chips - 1)], recv_sem.at[0, h])
        with scope("meet"):
            got = recv_v[h, :, :, dim:].astype(F32).reshape(chips * n_rows, 128).astype(BF16)
            tops = dot(got, pick_top, 1, 0).reshape(chips, n_rows, 128)
            totals = dot(got, pick_total, 1, 0).reshape(chips, n_rows, 128)
            factor = jnp.exp2(tops - jnp.max(tops, axis=0, keepdims=True))
            z = jnp.sum(factor * totals, axis=0)
            for d in range(dim // 128):
                cols = slice(d * 128, (d + 1) * 128)
                acc = jnp.sum(factor * recv_v[h, :, :, cols].astype(F32), axis=0)
                xs_v[:, :, cols] = (acc / z).reshape(2, per, 128)
            xin_v[h, core] = xs_v[core].astype(BF16)
            xout_v[h] = xs_v[other].astype(BF16)
        with scope("xs_exchange"):
            xs_copy = to_partner(xout_v.at[h], xin_v.at[h, core], 1, h)
            xs_copy.start()
            if h == 0:
                wait_bytes(win_v, l_sem.at[2])
                wait_bytes(win_v, recv_sem.at[5, 0])
            xs_copy.wait_recv()
        with scope("ffn"):
            ins = xin_v[h].astype(F32).reshape(n_rows, dim).astype(BF16)
            out = 0.0
            for m in range(2):
                hid = dot(ins, win_v[m], 1, 0)
                hid = (0.5 * hid * (1.0 + lax.erf(hid * 0.7071067811865476))).astype(BF16)
                out = out + dot(hid, wout_v[m], 1, 0)
            ys_v[h] = out.astype(BF16)
            ag_v[h, chip] = ys_v[h]
        with scope("send2"):
            for e in DIRECT:
                pltpu.make_async_remote_copy(ys_v.at[h], agx_v.at[h, chip], send_sem.at[3], recv_sem.at[3, h], device_id={"model": other, "seq": e}, device_id_type=MESH).start()
            for to in serve_first(0):
                pltpu.make_async_remote_copy(ys_v.at[h], ag_v.at[h, chip], send_sem.at[2], recv_sem.at[2, h], device_id={"seq": to}, device_id_type=MESH).start()

    mix_span("mix2", mix_next, n_batch)

    gives = []

    def spread(src, parity, h):
        for d in range(dim // 128):
            cols = slice(d * 128, (d + 1) * 128)
            unpack_v[d] = src[h, :, :, cols].astype(F32).reshape(chips * n_rows, 128)
            for r in range(n_rows):
                slots_v[parity, h * n_rows + r, :, cols] = unpack_v[d, pl.ds(r, chips, stride=n_rows), :].astype(BF16)

    def unpack(h):
        with scope("wait_ag"):
            wait_bytes(ag_v.at[h, pl.ds(1, chips - 1)], recv_sem.at[2, h])
        with scope("unpack"):
            spread(ag_v, core, h)
            mine = slots_v.at[core, pl.ds(h * n_rows, n_rows)]
            give = to_partner(mine, mine, 4, h)
            gives.append(give)

            @pl.when(jnp.logical_not(gets_both))
            def _():
                give.start()

            @pl.when(gets_both)
            def _():
                wait_bytes(agx_v.at[h], recv_sem.at[3, h])
                spread(agx_v, other, h)

    def settle(h):
        @pl.when(jnp.logical_not(gets_both))
        def _():
            gives[h].wait_recv()

    def mix_early(lo, hi):
        with scope("mix_early"):
            @pl.loop(lo, hi)
            def _(j):
                for span in spans:
                    y_v[j, span, :] = mix_rows(c_v, slots_v, left_v, j // per * half + j % per, j, span)

    unpack(0)
    with scope("wait_give"):
        settle(0)
    early_rows = jnp.where(gets_both, n_rows, n_rows // 2)
    mix_early(0, early_rows)
    unpack(1)
    mix_early(early_rows, n_rows)

    with scope("finish"):
        wait_bytes(send_v.at[:, pl.ds(1, chips - 1)], send_sem.at[0])
        wait_bytes(xout_v, send_sem.at[1])
        wait_bytes(ag_v.at[:, pl.ds(1, chips - 1)], send_sem.at[2])
        wait_bytes(agx_v.at[:, pl.ds(0, len(DIRECT))], send_sem.at[3])
        wait_bytes(win_v, send_sem.at[5])

        @pl.when(jnp.logical_not(gets_both))
        def _():
            wait_bytes(slots_v.at[core], send_sem.at[4])

        settle(1)


def mix_kernel(left, c, slots, y_v, y_hbm, rest_v, sems):
    n_batch, toks, _ = c.shape
    done, half = y_v.shape[0], n_batch // 2
    per = half // ROUNDS
    rows, parts = 256, 2

    def batch_of(j, h):
        return j // per * half + h * per + j % per

    for j in range(done):
        pltpu.make_async_copy(y_v.at[j], y_hbm.at[batch_of(j, 0)], sems.at[0]).start()

    @pl.loop(0, done)
    def _(j):
        b = batch_of(j, 1)
        for p in range(parts):
            for t in range(p * (toks // parts), (p + 1) * (toks // parts), rows):
                span = slice(t, t + rows)
                rest_v[j, span, :] = mix_rows(c, slots, left, b, done + j, span)
            span = pl.ds(p * (toks // parts), toks // parts)
            pltpu.make_async_copy(rest_v.at[j, span], y_hbm.at[b, span], sems.at[1]).start()

    pltpu.make_async_copy(y_v, y_hbm.at[pl.ds(0, done)], sems.at[0]).wait()
    pltpu.make_async_copy(rest_v, y_hbm.at[pl.ds(0, done)], sems.at[1]).wait()


def solution(mesh):
    def local_layer(tokens, lengths, slot_params, logit_scale, w_in, w_out):
        n_batch, toks, dim = tokens.shape
        slots = slot_params.shape[1]
        chips, half = slots // 2, n_batch // 2
        per = half // ROUNDS
        n_rows = 2 * per
        vmem = pl.BlockSpec(memory_space=pltpu.VMEM)
        hbm = pl.BlockSpec(memory_space=pltpu.HBM)
        dma = pltpu.SemaphoreType.DMA
        weights, slot_out, left, mixed = pl.pallas_call(
            moe_kernel,
            name="moe",
            out_shape=(pltpu.VMEM((n_batch, toks, slots), BF16), pltpu.VMEM((2, n_batch, chips, dim), BF16), pltpu.VMEM((n_batch, 128), jnp.int32), pltpu.VMEM((half, toks, dim), BF16)),
            in_specs=[hbm, pl.BlockSpec(memory_space=pltpu.SMEM)] + [hbm] * 4,
            out_specs=(vmem, vmem, vmem, vmem),
            scratch_shapes=[
                pltpu.SMEM((n_batch,), jnp.int32),
                pltpu.VMEM(slot_params.shape, BF16),
                pltpu.VMEM((n_batch, toks, dim), BF16),
                pltpu.VMEM(w_in.shape, BF16),
                pltpu.VMEM(w_out.shape, BF16),
                pltpu.VMEM((toks, dim), BF16),
                pltpu.VMEM((dim, slots), BF16),
                pltpu.VMEM((slots, dim), BF16),
                pltpu.VMEM((dim // 128, slots, 128), F32),
                pltpu.VMEM((slots, toks), F32),
                pltpu.VMEM((slots, toks), BF16),
                pltpu.VMEM((ROUNDS, dim // 128 + 1, chips * n_rows, 128), F32),
                pltpu.VMEM((ROUNDS, chips, n_rows, dim + 128), BF16),
                pltpu.VMEM((ROUNDS, chips, n_rows, dim + 128), BF16),
                pltpu.VMEM((2, per, dim), F32),
                pltpu.VMEM((ROUNDS, 2, per, dim), BF16),
                pltpu.VMEM((ROUNDS, per, dim), BF16),
                pltpu.VMEM((ROUNDS, n_rows, dim), BF16),
                pltpu.VMEM((ROUNDS, chips, n_rows, dim), BF16),
                pltpu.VMEM((ROUNDS, chips, n_rows, dim), BF16),
                pltpu.VMEM((dim // 128, chips * n_rows, 128), F32),
                dma((3,)), dma((3,)), dma((6,)), dma((6, ROUNDS)),
            ],
            compiler_params=pltpu.CompilerParams(collective_id=0, has_side_effects=True, vmem_limit_bytes=58380000),
        )(lengths, logit_scale, slot_params, tokens, w_in, w_out)
        return pl.pallas_call(
            mix_kernel,
            name="mix",
            out_shape=jax.ShapeDtypeStruct(tokens.shape, BF16),
            in_specs=[vmem, vmem, vmem, vmem],
            out_specs=hbm,
            scratch_shapes=[pltpu.VMEM((half, toks, dim), BF16), dma((2,))],
            compiler_params=pltpu.CompilerParams(vmem_limit_bytes=20 * 2**20),
        )(left, weights, slot_out, mixed)

    return jax.shard_map(local_layer, mesh=mesh, in_specs=(P("data", "seq", None), P("data"), P(), P(), P("seq", None, "model"), P("seq", "model", None)), out_specs=P("data", "seq", None), check_vma=False)
```

```python
import jax
import jax.numpy as jnp
from jax import lax
from jax.experimental import pallas as pl
from jax.experimental.pallas import tpu as pltpu
from jax.sharding import PartitionSpec as P

NORM_EPS = 1e-6
MESH = pl.DeviceIdType.MESH
SIDE = 4
F32, BF16 = jnp.float32, jnp.bfloat16
NEG = -1e30
LOG2E = 1.4426950408889634
ROUNDS = 2
DIRECT = (0, 1, 4)
scope = jax.named_scope


def dot(a, b, ca, cb):
    return lax.dot_general(a, b, (((ca,), (cb,)), ((), ())), preferred_element_type=F32)


def far_first():
    near = (0, 1, 2, 1)
    every = [(z, y, x) for z in range(SIDE) for y in range(SIDE) for x in range(SIDE)]
    return sorted(every[1:], key=lambda o: (-sum(near[i] for i in o), o))


def mix_rows(c, slots, left, b, at, span):
    outs = jnp.concatenate([slots[0, at], slots[1, at]], axis=0)
    out = dot(c[b, span, :], outs, 1, 0)
    pos = lax.broadcasted_iota(jnp.int32, out.shape, 0) + span.start
    bound = jnp.broadcast_to(left[pl.ds(b, 1), :1], out.shape)
    return jnp.where(pos < bound, out, 0.0).astype(BF16)


def moe_kernel(lens_hbm, scale, phi_hbm, x_hbm, win_hbm, wout_hbm, c_v, slots_v, left_v, y_v,
               lens, phi, x_v, win_v, wout_v, u_v, v_v, vt_v, tmp_v, lt_v, w_v, pack_v, send_v, recv_v,
               xs_v, xin_v, xout_v, ys_v, ag_v, agx_v, unpack_v,
               x_sem, l_sem, send_sem, recv_sem):
    n_batch, toks, dim = x_hbm.shape
    half = n_batch // 2
    per = half // ROUNDS
    slots = phi.shape[1]
    chips = slots // 2
    n_rows = 2 * per
    core = lax.axis_index("model")
    chip = lax.axis_index("seq")
    cz, cy, cx = chip // (SIDE * SIDE), (chip // SIDE) % SIDE, chip % SIDE
    first = core * half
    other = 1 - core

    def wait_bytes(ref, sem):
        pltpu.make_async_copy(ref, ref, sem).wait()

    def batch_of(q):
        return lax.rem(first + q, n_batch)

    def x_copy(q):
        return pltpu.make_async_copy(x_hbm.at[batch_of(q)], x_v.at[q], x_sem.at[0 if q == 0 else 1 if q < half else 2])

    loads = [pltpu.make_async_copy(a, b, l_sem.at[min(i, 2)]) for i, (a, b) in enumerate(
        ((phi_hbm, phi), (lens_hbm, lens), (win_hbm.at[core], win_v.at[core]), (wout_hbm.at[core], wout_v.at[core])))]

    def to_partner(src, dst, i, h):
        return pltpu.make_async_remote_copy(src, dst, send_sem.at[i], recv_sem.at[i, h], device_id={"model": other}, device_id_type=MESH)

    swaps = [to_partner(win_hbm.at[other], win_v.at[core], 5, 0), to_partner(wout_hbm.at[other], wout_v.at[core], 5, 0)]

    late = 8 * cz + 5 * cy + 4 * cx
    early = jnp.where(late <= 20, 1, 0)
    sums_first = per + (half - per) * early
    mix_first = early * jnp.where(late <= 4, 2, jnp.where(late <= 14, 1, 0))
    mix_between = mix_first + early * (2 - jnp.where(late <= 4, 1 - core, 0))
    mix_next = jnp.where(early == 1, mix_between + 2, 3)
    for load in loads[:2]:
        load.start()
    for q in range(per):
        x_copy(q).start()

    in_direct = sum((chip == e).astype(jnp.int32) for e in DIRECT)
    gets_both = in_direct == 1

    by_start = sorted(range(chips), key=lambda a: 8 * (a // 16) + 5 * (a // 4 % 4) + 4 * (a % 4))
    with scope("signal"):
        barrier = pltpu.get_barrier_semaphore()
        for to in [jnp.where(chip == a, by_start[-1], a) for a in by_start[:-1]]:
            pl.semaphore_signal(barrier, inc=1, device_id={"seq": to}, device_id_type=MESH)
        pl.semaphore_signal(barrier, inc=1, device_id={"model": other}, device_id_type=MESH)

        @pl.when(gets_both)
        def _():
            for to in [jnp.where(chip == a, by_start[-1], a) for a in by_start[:-1]]:
                pl.semaphore_signal(barrier, inc=1, device_id={"model": other, "seq": to}, device_id_type=MESH)

    at_z = [(cz + d) % SIDE * (SIDE * SIDE) for d in range(SIDE)]
    at_y = [(cy + d) % SIDE * SIDE for d in range(SIDE)]
    at_x = [(cx + d) % SIDE for d in range(SIDE)]
    peers = [at_z[z] + at_y[y] + at_x[x] for z, y, x in far_first()]

    with scope("phi"):
        for load in loads[:2]:
            load.wait()
        for q in range(per, n_batch):
            x_copy(q).start()
        for load in loads[2:]:
            load.start()
        g = scale[...] * LOG2E
        p32 = phi[...].astype(F32)
        unit = (p32 * lax.rsqrt(jnp.sum(p32 * p32, axis=0, keepdims=True) + NORM_EPS))
        for d in range(dim // 128):
            cols = slice(d * 128, (d + 1) * 128)
            tmp_v[d] = unit[cols, :].T
            for k in range(2):
                vt_v[k * chips:(k + 1) * chips, cols] = tmp_v[d, pl.ds(k, chips, stride=2), :].astype(BF16)
        v_v[...] = vt_v[...].astype(F32).T.astype(BF16)
        for b in range(n_batch):
            left_v[b:b + 1, :] = jnp.full((1, 128), lens[b] - chip * toks, jnp.int32)

    def unit_rows(q, u, start, size):
        for t in range(start, start + size, 64):
            span = slice(t, t + 64)
            part = x_v[q, span, :].astype(F32)
            norm = lax.rsqrt(jnp.sum(part * part, axis=1, keepdims=True) + NORM_EPS)
            u[span, :] = (x_v[q, span, :].astype(F32) * norm).astype(BF16)

    rows = 256
    lane = lax.broadcasted_iota(jnp.int32, (slots, 128), 1)
    spans = [slice(t, t + rows) for t in range(0, toks, rows)]

    def dispatch(q):
        @pl.when(q == 1)
        def _():
            wait_bytes(x_v.at[pl.ds(1, half - 1)], x_sem.at[1])
        u, lt, w_b = u_v, lt_v, w_v
        h, i = q // per, q % per
        left = lens[batch_of(q)] - chip * toks
        bias = jnp.where(lax.broadcasted_iota(jnp.int32, (1, toks), 1) < left, 0.0, NEG)
        top = jnp.full((slots, rows), NEG, F32)
        for span in spans:
            unit_rows(q, u, span.start, rows)
            lg = g * dot(vt_v[...], u[span, :], 1, 1) + bias[:, span]
            lt[:, span] = lg
            top = jnp.maximum(top, lg)
        top = jnp.max(top, axis=1, keepdims=True)
        total = jnp.zeros((slots, rows), F32)
        for span in spans:
            w = jnp.exp2(lt[:, span] - top)
            total = total + w
            w_b[:, span] = w.astype(BF16)
        total = jnp.sum(total, axis=1, keepdims=True)
        sums = dot(w_b[...], x_v[q], 1, 0)
        stat = jnp.zeros((slots, 128), F32)
        for pos, val in ((0, top), (3, total)):
            rest = val
            for j in range(3):
                piece = rest.astype(BF16).astype(F32)
                rest = rest - piece
                stat = jnp.where(lane == pos + j, piece, stat)
        for k in range(2):
            dst = pl.ds(k * per + i, chips, stride=n_rows)
            for d in range(dim // 128):
                pack_v[h, d, dst, :] = sums[k * chips:(k + 1) * chips, d * 128:(d + 1) * 128]
            pack_v[h, dim // 128, dst, :] = stat[k * chips:(k + 1) * chips, :]

    def serve_first(*favoured):
        order = list(peers)
        for a in reversed(favoured):
            last = order[-1]
            order = [jnp.where(chip == a, last, a)] + [jnp.where(to == a, last, to) for to in order[:-1]]
        return order

    def send_sums(h):
        for d in range(dim // 128 + 1):
            send_v[h, :, :, d * 128:(d + 1) * 128] = pack_v[h, d].astype(BF16).reshape(chips, n_rows, 128)
        recv_v[h, chip] = send_v[h, chip]
        for to in serve_first(63):
            pltpu.make_async_remote_copy(send_v.at[h, to], recv_v.at[h, chip], send_sem.at[0], recv_sem.at[0, h], device_id={"seq": to}, device_id_type=MESH).start()

    def mix_weights(q):
        b = batch_of(q)
        for span in spans:
            unit_rows(q, u_v, span.start, rows)
            lg = g * dot(u_v[span, :], v_v[...], 1, 0)
            e = jnp.exp2(lg - jnp.max(lg, axis=1, keepdims=True))
            c_v[b, span, :] = (e / jnp.sum(e, axis=1, keepdims=True)).astype(BF16)

    def mix_span(name, lo, hi):
        with scope(name):
            @pl.loop(lo, hi)
            def _(q):
                mix_weights(q)

    with scope("dispatch"):
        wait_bytes(x_v.at[0], x_sem.at[0])

        @pl.loop(0, sums_first)
        def _(q):
            dispatch(q)
    mix_span("mix0", 0, mix_first)
    with scope("barrier"):
        pl.semaphore_wait(barrier, chips + len(DIRECT) - in_direct)
    with scope("send"):
        send_sums(0)
        for swap in swaps:
            swap.start()
    with scope("dispatch2"):
        @pl.loop(sums_first, half)
        def _(q):
            dispatch(q)
    mix_span("mix01", mix_first, mix_between)
    with scope("sendb"):
        send_sums(1)
    wait_bytes(x_v.at[pl.ds(half, n_batch - half)], x_sem.at[2])
    mix_span("mix1", mix_between, mix_next)

    sel_row = lax.broadcasted_iota(jnp.int32, (128, 128), 0)
    pick_top = (sel_row < 3).astype(F32).astype(BF16)
    pick_total = ((sel_row >= 3) & (sel_row < 6)).astype(F32).astype(BF16)

    for h in range(ROUNDS):
        with scope("wait_a2a"):
            wait_bytes(recv_v.at[h, pl.ds(1, chips - 1)], recv_sem.at[0, h])
        with scope("meet"):
            got = recv_v[h, :, :, dim:].astype(F32).reshape(chips * n_rows, 128).astype(BF16)
            tops = dot(got, pick_top, 1, 0).reshape(chips, n_rows, 128)
            totals = dot(got, pick_total, 1, 0).reshape(chips, n_rows, 128)
            factor = jnp.exp2(tops - jnp.max(tops, axis=0, keepdims=True))
            z = jnp.sum(factor * totals, axis=0)
            for d in range(dim // 128):
                cols = slice(d * 128, (d + 1) * 128)
                acc = jnp.sum(factor * recv_v[h, :, :, cols].astype(F32), axis=0)
                xs_v[:, :, cols] = (acc / z).reshape(2, per, 128)
            xin_v[h, core] = xs_v[core].astype(BF16)
            xout_v[h] = xs_v[other].astype(BF16)
        with scope("xs_exchange"):
            xs_copy = to_partner(xout_v.at[h], xin_v.at[h, core], 1, h)
            xs_copy.start()
            if h == 0:
                wait_bytes(win_v, l_sem.at[2])
                wait_bytes(win_v, recv_sem.at[5, 0])
            xs_copy.wait_recv()
        with scope("ffn"):
            ins = xin_v[h].astype(F32).reshape(n_rows, dim).astype(BF16)
            out = 0.0
            for m in range(2):
                hid = dot(ins, win_v[m], 1, 0)
                hid = (0.5 * hid * (1.0 + lax.erf(hid * 0.7071067811865476))).astype(BF16)
                out = out + dot(hid, wout_v[m], 1, 0)
            ys_v[h] = out.astype(BF16)
            ag_v[h, chip] = ys_v[h]
        with scope("send2"):
            for e in DIRECT:
                pltpu.make_async_remote_copy(ys_v.at[h], agx_v.at[h, chip], send_sem.at[3], recv_sem.at[3, h], device_id={"model": other, "seq": e}, device_id_type=MESH).start()
            for to in serve_first(0):
                pltpu.make_async_remote_copy(ys_v.at[h], ag_v.at[h, chip], send_sem.at[2], recv_sem.at[2, h], device_id={"seq": to}, device_id_type=MESH).start()

    mix_span("mix2", mix_next, n_batch)

    gives = []

    def spread(src, parity, h):
        for d in range(dim // 128):
            cols = slice(d * 128, (d + 1) * 128)
            unpack_v[d] = src[h, :, :, cols].astype(F32).reshape(chips * n_rows, 128)
            for r in range(n_rows):
                slots_v[parity, h * n_rows + r, :, cols] = unpack_v[d, pl.ds(r, chips, stride=n_rows), :].astype(BF16)

    def unpack(h):
        with scope("wait_ag"):
            wait_bytes(ag_v.at[h, pl.ds(1, chips - 1)], recv_sem.at[2, h])
        with scope("unpack"):
            spread(ag_v, core, h)
            mine = slots_v.at[core, pl.ds(h * n_rows, n_rows)]
            give = to_partner(mine, mine, 4, h)
            gives.append(give)

            @pl.when(jnp.logical_not(gets_both))
            def _():
                give.start()

            @pl.when(gets_both)
            def _():
                wait_bytes(agx_v.at[h], recv_sem.at[3, h])
                spread(agx_v, other, h)

    def settle(h):
        @pl.when(jnp.logical_not(gets_both))
        def _():
            gives[h].wait_recv()

    def mix_early(lo, hi):
        with scope("mix_early"):
            @pl.loop(lo, hi)
            def _(j):
                for span in spans:
                    y_v[j, span, :] = mix_rows(c_v, slots_v, left_v, j // per * half + j % per, j, span)

    unpack(0)
    with scope("wait_give"):
        settle(0)
    early_rows = jnp.where(gets_both, n_rows, n_rows // 2)
    mix_early(0, early_rows)
    unpack(1)
    mix_early(early_rows, n_rows)

    with scope("finish"):
        wait_bytes(send_v.at[:, pl.ds(1, chips - 1)], send_sem.at[0])
        wait_bytes(xout_v, send_sem.at[1])
        wait_bytes(ag_v.at[:, pl.ds(1, chips - 1)], send_sem.at[2])
        wait_bytes(agx_v.at[:, pl.ds(0, len(DIRECT))], send_sem.at[3])
        wait_bytes(win_v, send_sem.at[5])

        @pl.when(jnp.logical_not(gets_both))
        def _():
            wait_bytes(slots_v.at[core], send_sem.at[4])

        settle(1)


def mix_kernel(left, c, slots, y_v, y_hbm, rest_v, sems):
    n_batch, toks, _ = c.shape
    done, half = y_v.shape[0], n_batch // 2
    per = half // ROUNDS
    rows, parts = 256, 2

    def batch_of(j, h):
        return j // per * half + h * per + j % per

    for j in range(done):
        pltpu.make_async_copy(y_v.at[j], y_hbm.at[batch_of(j, 0)], sems.at[0]).start()

    @pl.loop(0, done)
    def _(j):
        b = batch_of(j, 1)
        for p in range(parts):
            for t in range(p * (toks // parts), (p + 1) * (toks // parts), rows):
                span = slice(t, t + rows)
                rest_v[j, span, :] = mix_rows(c, slots, left, b, done + j, span)
            span = pl.ds(p * (toks // parts), toks // parts)
            pltpu.make_async_copy(rest_v.at[j, span], y_hbm.at[b, span], sems.at[1]).start()

    pltpu.make_async_copy(y_v, y_hbm.at[pl.ds(0, done)], sems.at[0]).wait()
    pltpu.make_async_copy(rest_v, y_hbm.at[pl.ds(0, done)], sems.at[1]).wait()


def solution(mesh):
    def local_layer(tokens, lengths, slot_params, logit_scale, w_in, w_out):
        n_batch, toks, dim = tokens.shape
        slots = slot_params.shape[1]
        chips, half = slots // 2, n_batch // 2
        per = half // ROUNDS
        n_rows = 2 * per
        vmem = pl.BlockSpec(memory_space=pltpu.VMEM)
        hbm = pl.BlockSpec(memory_space=pltpu.HBM)
        dma = pltpu.SemaphoreType.DMA
        weights, slot_out, left, mixed = pl.pallas_call(
            moe_kernel,
            name="moe",
            out_shape=(pltpu.VMEM((n_batch, toks, slots), BF16), pltpu.VMEM((2, n_batch, chips, dim), BF16), pltpu.VMEM((n_batch, 128), jnp.int32), pltpu.VMEM((half, toks, dim), BF16)),
            in_specs=[hbm, pl.BlockSpec(memory_space=pltpu.SMEM)] + [hbm] * 4,
            out_specs=(vmem, vmem, vmem, vmem),
            scratch_shapes=[
                pltpu.SMEM((n_batch,), jnp.int32),
                pltpu.VMEM(slot_params.shape, BF16),
                pltpu.VMEM((n_batch, toks, dim), BF16),
                pltpu.VMEM(w_in.shape, BF16),
                pltpu.VMEM(w_out.shape, BF16),
                pltpu.VMEM((toks, dim), BF16),
                pltpu.VMEM((dim, slots), BF16),
                pltpu.VMEM((slots, dim), BF16),
                pltpu.VMEM((dim // 128, slots, 128), F32),
                pltpu.VMEM((slots, toks), F32),
                pltpu.VMEM((slots, toks), BF16),
                pltpu.VMEM((ROUNDS, dim // 128 + 1, chips * n_rows, 128), F32),
                pltpu.VMEM((ROUNDS, chips, n_rows, dim + 128), BF16),
                pltpu.VMEM((ROUNDS, chips, n_rows, dim + 128), BF16),
                pltpu.VMEM((2, per, dim), F32),
                pltpu.VMEM((ROUNDS, 2, per, dim), BF16),
                pltpu.VMEM((ROUNDS, per, dim), BF16),
                pltpu.VMEM((ROUNDS, n_rows, dim), BF16),
                pltpu.VMEM((ROUNDS, chips, n_rows, dim), BF16),
                pltpu.VMEM((ROUNDS, chips, n_rows, dim), BF16),
                pltpu.VMEM((dim // 128, chips * n_rows, 128), F32),
                dma((3,)), dma((3,)), dma((6,)), dma((6, ROUNDS)),
            ],
            compiler_params=pltpu.CompilerParams(collective_id=0, has_side_effects=True, vmem_limit_bytes=58380000),
        )(lengths, logit_scale, slot_params, tokens, w_in, w_out)
        return pl.pallas_call(
            mix_kernel,
            name="mix",
            out_shape=jax.ShapeDtypeStruct(tokens.shape, BF16),
            in_specs=[vmem, vmem, vmem, vmem],
            out_specs=hbm,
            scratch_shapes=[pltpu.VMEM((half, toks, dim), BF16), dma((2,))],
            compiler_params=pltpu.CompilerParams(vmem_limit_bytes=20 * 2**20),
        )(left, weights, slot_out, mixed)

    return jax.shard_map(local_layer, mesh=mesh, in_specs=(P("data", "seq", None), P("data"), P(), P(), P("seq", None, "model"), P("seq", "model", None)), out_specs=P("data", "seq", None), check_vma=False)
```

```python
import jax
import jax.numpy as jnp
from jax import lax
from jax.experimental import pallas as pl
from jax.experimental.pallas import tpu as pltpu
from jax.sharding import PartitionSpec as P

NORM_EPS = 1e-6
MESH = pl.DeviceIdType.MESH
SIDE = 4
F32, BF16 = jnp.float32, jnp.bfloat16
NEG = -1e30
LOG2E = 1.4426950408889634
ROUNDS = 2
DIRECT = (0, 1, 4)
scope = jax.named_scope


def dot(a, b, ca, cb):
    return lax.dot_general(a, b, (((ca,), (cb,)), ((), ())), preferred_element_type=F32)


def far_first():
    near = (0, 1, 2, 1)
    every = [(z, y, x) for z in range(SIDE) for y in range(SIDE) for x in range(SIDE)]
    return sorted(every[1:], key=lambda o: (-sum(near[i] for i in o), o))


def mix_rows(c, slots, left, b, at, span):
    outs = jnp.concatenate([slots[0, at], slots[1, at]], axis=0)
    out = dot(c[b, span, :], outs, 1, 0)
    pos = lax.broadcasted_iota(jnp.int32, out.shape, 0) + span.start
    bound = jnp.broadcast_to(left[pl.ds(b, 1), :1], out.shape)
    return jnp.where(pos < bound, out, 0.0).astype(BF16)


def moe_kernel(lens_hbm, scale, phi_hbm, x_hbm, win_hbm, wout_hbm, c_v, slots_v, left_v, y_v,
               lens, phi, x_v, win_v, wout_v, u_v, v_v, vt_v, tmp_v, lt_v, w_v, pack_v, send_v, recv_v,
               xs_v, xin_v, xout_v, ys_v, ag_v, agx_v, unpack_v,
               x_sem, l_sem, send_sem, recv_sem):
    n_batch, toks, dim = x_hbm.shape
    half = n_batch // 2
    per = half // ROUNDS
    slots = phi.shape[1]
    chips = slots // 2
    n_rows = 2 * per
    core = lax.axis_index("model")
    chip = lax.axis_index("seq")
    cz, cy, cx = chip // (SIDE * SIDE), (chip // SIDE) % SIDE, chip % SIDE
    first = core * half
    other = 1 - core

    def wait_bytes(ref, sem):
        pltpu.make_async_copy(ref, ref, sem).wait()

    def batch_of(q):
        return lax.rem(first + q, n_batch)

    def x_copy(q):
        return pltpu.make_async_copy(x_hbm.at[batch_of(q)], x_v.at[q], x_sem.at[0 if q == 0 else 1 if q < half else 2])

    loads = [pltpu.make_async_copy(a, b, l_sem.at[min(i, 2)]) for i, (a, b) in enumerate(
        ((phi_hbm, phi), (lens_hbm, lens), (win_hbm.at[core], win_v.at[core]), (wout_hbm.at[core], wout_v.at[core])))]

    def to_partner(src, dst, i, h):
        return pltpu.make_async_remote_copy(src, dst, send_sem.at[i], recv_sem.at[i, h], device_id={"model": other}, device_id_type=MESH)

    swaps = [to_partner(win_hbm.at[other], win_v.at[core], 5, 0), to_partner(wout_hbm.at[other], wout_v.at[core], 5, 0)]

    late = 8 * cz + 5 * cy + 4 * cx
    early = jnp.where(late <= 20, 1, 0)
    sums_first = per + (half - per) * early
    mix_first = early * jnp.where(late <= 4, 2, jnp.where(late <= 14, 1, 0))
    mix_between = mix_first + early * (2 - jnp.where(late <= 4, 1 - core, 0))
    mix_next = jnp.where(early == 1, mix_between + 2, 3)
    for load in loads[:2]:
        load.start()
    for q in range(per):
        x_copy(q).start()

    in_direct = sum((chip == e).astype(jnp.int32) for e in DIRECT)
    gets_both = in_direct == 1

    by_start = sorted(range(chips), key=lambda a: 8 * (a // 16) + 5 * (a // 4 % 4) + 4 * (a % 4))
    with scope("signal"):
        barrier = pltpu.get_barrier_semaphore()
        for to in [jnp.where(chip == a, by_start[-1], a) for a in by_start[:-1]]:
            pl.semaphore_signal(barrier, inc=1, device_id={"seq": to}, device_id_type=MESH)
        pl.semaphore_signal(barrier, inc=1, device_id={"model": other}, device_id_type=MESH)

        @pl.when(gets_both)
        def _():
            for to in [jnp.where(chip == a, by_start[-1], a) for a in by_start[:-1]]:
                pl.semaphore_signal(barrier, inc=1, device_id={"model": other, "seq": to}, device_id_type=MESH)

    at_z = [(cz + d) % SIDE * (SIDE * SIDE) for d in range(SIDE)]
    at_y = [(cy + d) % SIDE * SIDE for d in range(SIDE)]
    at_x = [(cx + d) % SIDE for d in range(SIDE)]
    peers = [at_z[z] + at_y[y] + at_x[x] for z, y, x in far_first()]

    with scope("phi"):
        for load in loads[:2]:
            load.wait()
        for q in range(per, n_batch):
            x_copy(q).start()
        for load in loads[2:]:
            load.start()
        g = scale[...] * LOG2E
        p32 = phi[...].astype(F32)
        unit = (p32 * lax.rsqrt(jnp.sum(p32 * p32, axis=0, keepdims=True) + NORM_EPS))
        for d in range(dim // 128):
            cols = slice(d * 128, (d + 1) * 128)
            tmp_v[d] = unit[cols, :].T
            for k in range(2):
                vt_v[k * chips:(k + 1) * chips, cols] = tmp_v[d, pl.ds(k, chips, stride=2), :].astype(BF16)
        v_v[...] = vt_v[...].astype(F32).T.astype(BF16)
        for b in range(n_batch):
            left_v[b:b + 1, :] = jnp.full((1, 128), lens[b] - chip * toks, jnp.int32)

    def unit_rows(q, u, start, size):
        for t in range(start, start + size, 64):
            span = slice(t, t + 64)
            part = x_v[q, span, :].astype(F32)
            norm = lax.rsqrt(jnp.sum(part * part, axis=1, keepdims=True) + NORM_EPS)
            u[span, :] = (x_v[q, span, :].astype(F32) * norm).astype(BF16)

    rows = 256
    lane = lax.broadcasted_iota(jnp.int32, (slots, 128), 1)
    spans = [slice(t, t + rows) for t in range(0, toks, rows)]

    def dispatch(q):
        @pl.when(q == 1)
        def _():
            wait_bytes(x_v.at[pl.ds(1, half - 1)], x_sem.at[1])
        u, lt, w_b = u_v, lt_v, w_v
        h, i = q // per, q % per
        left = lens[batch_of(q)] - chip * toks
        bias = jnp.where(lax.broadcasted_iota(jnp.int32, (1, toks), 1) < left, 0.0, NEG)
        top = jnp.full((slots, rows), NEG, F32)
        for span in spans:
            unit_rows(q, u, span.start, rows)
            lg = g * dot(vt_v[...], u[span, :], 1, 1) + bias[:, span]
            lt[:, span] = lg
            top = jnp.maximum(top, lg)
        top = jnp.max(top, axis=1, keepdims=True)
        total = jnp.zeros((slots, rows), F32)
        for span in spans:
            w = jnp.exp2(lt[:, span] - top)
            total = total + w
            w_b[:, span] = w.astype(BF16)
        total = jnp.sum(total, axis=1, keepdims=True)
        sums = dot(w_b[...], x_v[q], 1, 0)
        stat = jnp.zeros((slots, 128), F32)
        for pos, val in ((0, top), (3, total)):
            rest = val
            for j in range(3):
                piece = rest.astype(BF16).astype(F32)
                rest = rest - piece
                stat = jnp.where(lane == pos + j, piece, stat)
        for k in range(2):
            dst = pl.ds(k * per + i, chips, stride=n_rows)
            for d in range(dim // 128):
                pack_v[h, d, dst, :] = sums[k * chips:(k + 1) * chips, d * 128:(d + 1) * 128]
            pack_v[h, dim // 128, dst, :] = stat[k * chips:(k + 1) * chips, :]

    def serve_first(*favoured):
        order = list(peers)
        for a in reversed(favoured):
            last = order[-1]
            order = [jnp.where(chip == a, last, a)] + [jnp.where(to == a, last, to) for to in order[:-1]]
        return order

    def send_sums(h):
        for d in range(dim // 128 + 1):
            send_v[h, :, :, d * 128:(d + 1) * 128] = pack_v[h, d].astype(BF16).reshape(chips, n_rows, 128)
        recv_v[h, chip] = send_v[h, chip]
        for to in serve_first(63):
            pltpu.make_async_remote_copy(send_v.at[h, to], recv_v.at[h, chip], send_sem.at[0], recv_sem.at[0, h], device_id={"seq": to}, device_id_type=MESH).start()

    def mix_weights(q):
        b = batch_of(q)
        for span in spans:
            unit_rows(q, u_v, span.start, rows)
            lg = g * dot(u_v[span, :], v_v[...], 1, 0)
            e = jnp.exp2(lg - jnp.max(lg, axis=1, keepdims=True))
            c_v[b, span, :] = (e / jnp.sum(e, axis=1, keepdims=True)).astype(BF16)

    def mix_span(name, lo, hi):
        with scope(name):
            @pl.loop(lo, hi)
            def _(q):
                mix_weights(q)

    with scope("dispatch"):
        wait_bytes(x_v.at[0], x_sem.at[0])

        @pl.loop(0, sums_first)
        def _(q):
            dispatch(q)
    mix_span("mix0", 0, mix_first)
    with scope("barrier"):
        pl.semaphore_wait(barrier, chips + len(DIRECT) - in_direct)
    with scope("send"):
        send_sums(0)
        for swap in swaps:
            swap.start()
    with scope("dispatch2"):
        @pl.loop(sums_first, half)
        def _(q):
            dispatch(q)
    mix_span("mix01", mix_first, mix_between)
    with scope("sendb"):
        send_sums(1)
    wait_bytes(x_v.at[pl.ds(half, n_batch - half)], x_sem.at[2])
    mix_span("mix1", mix_between, mix_next)

    sel_row = lax.broadcasted_iota(jnp.int32, (128, 128), 0)
    pick_top = (sel_row < 3).astype(F32).astype(BF16)
    pick_total = ((sel_row >= 3) & (sel_row < 6)).astype(F32).astype(BF16)

    for h in range(ROUNDS):
        with scope("wait_a2a"):
            wait_bytes(recv_v.at[h, pl.ds(1, chips - 1)], recv_sem.at[0, h])
        with scope("meet"):
            got = recv_v[h, :, :, dim:].astype(F32).reshape(chips * n_rows, 128).astype(BF16)
            tops = dot(got, pick_top, 1, 0).reshape(chips, n_rows, 128)
            totals = dot(got, pick_total, 1, 0).reshape(chips, n_rows, 128)
            factor = jnp.exp2(tops - jnp.max(tops, axis=0, keepdims=True))
            z = jnp.sum(factor * totals, axis=0)
            for d in range(dim // 128):
                cols = slice(d * 128, (d + 1) * 128)
                acc = jnp.sum(factor * recv_v[h, :, :, cols].astype(F32), axis=0)
                xs_v[:, :, cols] = (acc / z).reshape(2, per, 128)
            xin_v[h, core] = xs_v[core].astype(BF16)
            xout_v[h] = xs_v[other].astype(BF16)
        with scope("xs_exchange"):
            xs_copy = to_partner(xout_v.at[h], xin_v.at[h, core], 1, h)
            xs_copy.start()
            if h == 0:
                wait_bytes(win_v, l_sem.at[2])
                wait_bytes(win_v, recv_sem.at[5, 0])
            xs_copy.wait_recv()
        with scope("ffn"):
            ins = xin_v[h].astype(F32).reshape(n_rows, dim).astype(BF16)
            out = 0.0
            for m in range(2):
                hid = dot(ins, win_v[m], 1, 0)
                hid = (0.5 * hid * (1.0 + lax.erf(hid * 0.7071067811865476))).astype(BF16)
                out = out + dot(hid, wout_v[m], 1, 0)
            ys_v[h] = out.astype(BF16)
            ag_v[h, chip] = ys_v[h]
        with scope("send2"):
            for n, to in enumerate(serve_first(0)):
                pltpu.make_async_remote_copy(ys_v.at[h], ag_v.at[h, chip], send_sem.at[2], recv_sem.at[2, h], device_id={"seq": to}, device_id_type=MESH).start()
                if n == 0:
                    for e in DIRECT:
                        pltpu.make_async_remote_copy(ys_v.at[h], agx_v.at[h, chip], send_sem.at[3], recv_sem.at[3, h], device_id={"model": other, "seq": e}, device_id_type=MESH).start()

    mix_span("mix2", mix_next, n_batch)

    gives = []

    def spread(src, parity, h):
        for d in range(dim // 128):
            cols = slice(d * 128, (d + 1) * 128)
            unpack_v[d] = src[h, :, :, cols].astype(F32).reshape(chips * n_rows, 128)
            for r in range(n_rows):
                slots_v[parity, h * n_rows + r, :, cols] = unpack_v[d, pl.ds(r, chips, stride=n_rows), :].astype(BF16)

    def unpack(h):
        with scope("wait_ag"):
            wait_bytes(ag_v.at[h, pl.ds(1, chips - 1)], recv_sem.at[2, h])
        with scope("unpack"):
            spread(ag_v, core, h)
            mine = slots_v.at[core, pl.ds(h * n_rows, n_rows)]
            give = to_partner(mine, mine, 4, h)
            gives.append(give)

            @pl.when(jnp.logical_not(gets_both))
            def _():
                give.start()

            @pl.when(gets_both)
            def _():
                wait_bytes(agx_v.at[h], recv_sem.at[3, h])
                spread(agx_v, other, h)

    def settle(h):
        @pl.when(jnp.logical_not(gets_both))
        def _():
            gives[h].wait_recv()

    def mix_early(lo, hi):
        with scope("mix_early"):
            @pl.loop(lo, hi)
            def _(j):
                for span in spans:
                    y_v[j, span, :] = mix_rows(c_v, slots_v, left_v, j // per * half + j % per, j, span)

    unpack(0)
    with scope("wait_give"):
        settle(0)
    early_rows = jnp.where(gets_both, n_rows, n_rows // 2)
    mix_early(0, early_rows)
    unpack(1)
    mix_early(early_rows, n_rows)

    with scope("finish"):
        wait_bytes(send_v.at[:, pl.ds(1, chips - 1)], send_sem.at[0])
        wait_bytes(xout_v, send_sem.at[1])
        wait_bytes(ag_v.at[:, pl.ds(1, chips - 1)], send_sem.at[2])
        wait_bytes(agx_v.at[:, pl.ds(0, len(DIRECT))], send_sem.at[3])
        wait_bytes(win_v, send_sem.at[5])

        @pl.when(jnp.logical_not(gets_both))
        def _():
            wait_bytes(slots_v.at[core], send_sem.at[4])

        settle(1)


def mix_kernel(left, c, slots, y_v, y_hbm, rest_v, sems):
    n_batch, toks, _ = c.shape
    done, half = y_v.shape[0], n_batch // 2
    per = half // ROUNDS
    rows, parts = 256, 2

    def batch_of(j, h):
        return j // per * half + h * per + j % per

    for j in range(done):
        pltpu.make_async_copy(y_v.at[j], y_hbm.at[batch_of(j, 0)], sems.at[0]).start()

    @pl.loop(0, done)
    def _(j):
        b = batch_of(j, 1)
        for p in range(parts):
            for t in range(p * (toks // parts), (p + 1) * (toks // parts), rows):
                span = slice(t, t + rows)
                rest_v[j, span, :] = mix_rows(c, slots, left, b, done + j, span)
            span = pl.ds(p * (toks // parts), toks // parts)
            pltpu.make_async_copy(rest_v.at[j, span], y_hbm.at[b, span], sems.at[1]).start()

    pltpu.make_async_copy(y_v, y_hbm.at[pl.ds(0, done)], sems.at[0]).wait()
    pltpu.make_async_copy(rest_v, y_hbm.at[pl.ds(0, done)], sems.at[1]).wait()


def solution(mesh):
    def local_layer(tokens, lengths, slot_params, logit_scale, w_in, w_out):
        n_batch, toks, dim = tokens.shape
        slots = slot_params.shape[1]
        chips, half = slots // 2, n_batch // 2
        per = half // ROUNDS
        n_rows = 2 * per
        vmem = pl.BlockSpec(memory_space=pltpu.VMEM)
        hbm = pl.BlockSpec(memory_space=pltpu.HBM)
        dma = pltpu.SemaphoreType.DMA
        weights, slot_out, left, mixed = pl.pallas_call(
            moe_kernel,
            name="moe",
            out_shape=(pltpu.VMEM((n_batch, toks, slots), BF16), pltpu.VMEM((2, n_batch, chips, dim), BF16), pltpu.VMEM((n_batch, 128), jnp.int32), pltpu.VMEM((half, toks, dim), BF16)),
            in_specs=[hbm, pl.BlockSpec(memory_space=pltpu.SMEM)] + [hbm] * 4,
            out_specs=(vmem, vmem, vmem, vmem),
            scratch_shapes=[
                pltpu.SMEM((n_batch,), jnp.int32),
                pltpu.VMEM(slot_params.shape, BF16),
                pltpu.VMEM((n_batch, toks, dim), BF16),
                pltpu.VMEM(w_in.shape, BF16),
                pltpu.VMEM(w_out.shape, BF16),
                pltpu.VMEM((toks, dim), BF16),
                pltpu.VMEM((dim, slots), BF16),
                pltpu.VMEM((slots, dim), BF16),
                pltpu.VMEM((dim // 128, slots, 128), F32),
                pltpu.VMEM((slots, toks), F32),
                pltpu.VMEM((slots, toks), BF16),
                pltpu.VMEM((ROUNDS, dim // 128 + 1, chips * n_rows, 128), F32),
                pltpu.VMEM((ROUNDS, chips, n_rows, dim + 128), BF16),
                pltpu.VMEM((ROUNDS, chips, n_rows, dim + 128), BF16),
                pltpu.VMEM((2, per, dim), F32),
                pltpu.VMEM((ROUNDS, 2, per, dim), BF16),
                pltpu.VMEM((ROUNDS, per, dim), BF16),
                pltpu.VMEM((ROUNDS, n_rows, dim), BF16),
                pltpu.VMEM((ROUNDS, chips, n_rows, dim), BF16),
                pltpu.VMEM((ROUNDS, chips, n_rows, dim), BF16),
                pltpu.VMEM((dim // 128, chips * n_rows, 128), F32),
                dma((3,)), dma((3,)), dma((6,)), dma((6, ROUNDS)),
            ],
            compiler_params=pltpu.CompilerParams(collective_id=0, has_side_effects=True, vmem_limit_bytes=58380000),
        )(lengths, logit_scale, slot_params, tokens, w_in, w_out)
        return pl.pallas_call(
            mix_kernel,
            name="mix",
            out_shape=jax.ShapeDtypeStruct(tokens.shape, BF16),
            in_specs=[vmem, vmem, vmem, vmem],
            out_specs=hbm,
            scratch_shapes=[pltpu.VMEM((half, toks, dim), BF16), dma((2,))],
            compiler_params=pltpu.CompilerParams(vmem_limit_bytes=20 * 2**20),
        )(left, weights, slot_out, mixed)

    return jax.shard_map(local_layer, mesh=mesh, in_specs=(P("data", "seq", None), P("data"), P(), P(), P("seq", None, "model"), P("seq", "model", None)), out_specs=P("data", "seq", None), check_vma=False)
```
